256 devices in a mesh: lat: 64 (over z, y, core), tok: 4 (over x).
Axes of the slice: x: 4, y: 4, z: 8, core: 2. Of those that a mesh axis runs over, the one named last changes fastest.
Arguments:
- coefficients: bfloat16 [2048, 16, 128], P(('lat', 'tok')), may hold values from 0 to 2
- block_ids: int32 [2048, 16], P(('lat', 'tok')), may hold values from 0 to 1023, all different within a row; in each aligned block of 32 rows (0 to 31, 32 to 63, ...) at most 2 rows name the same one
- counts: int32 [2048], P(('lat', 'tok')), may hold values from 10 to 16
- decoder: bfloat16 [1, 131072, 5120], P(None, 'lat', 'tok'), may hold values from -0.125 to 0.125
- bias: float32 [1, 5120], P(None, 'tok'), may hold values from -3 to 3
Outputs:
- recon: bfloat16 [1, 2048, 5120], P(None, 'lat', 'tok')
The draws below stay inside these ranges and needn't reach their ends.
Inputs may be any that keep to these rules, and one draw needn't show every extreme that they name: `block_ids`: the 16 slots of a token name different blocks. Among the tokens of one index of lat (aligned blocks of 32 rows), no block is named by more than 2 slots, live or padding, and some block is named by exactly 2. `counts`: slots below a token's count are live, the others padding.
All inputs are finite; a program needn't handle non-finite values.
Results may differ from the reference program's by a relative error of at most 0.001.
Values may be sent and summed in bfloat16 or wider, within the bound.
No kernel may reach another device: no remote copies, remote signals or barrier semaphores. Data moves between devices by JAX's collectives and lax.ppermute only.
A program may use at most 128 MiB of HBM per device.

```python
import math
import jax
import jax.numpy as jnp
import numpy as np
from jax import lax

D = 5120
BLOCKS = 1024
BLOCK = 128
ACTIVE = 16
LAYERS = 1
TOK_LAT = 32
TOKENS = 2048
LATENTS = 131072
MOST = 2
N_LAT = 64


def set_ends(array, stream_key, smallest, high):
    spot = [jax.random.randint(jax.random.fold_in(stream_key, axis), (), 0, length) for axis, length in enumerate(array.shape)]
    widest = array.shape.index(max(array.shape))
    next_to = spot[:widest] + [(spot[widest] + 1) % array.shape[widest]] + spot[widest + 1:]
    return array.at[tuple(spot)].set(smallest).at[tuple(next_to)].set(high)


def block_scale(key, shape, shards, least, high):
    gain = 1.0
    for dim, shards_of in shards:
        steps = jax.random.uniform(jax.random.fold_in(jax.random.fold_in(key, 6), dim), (shards_of,), jnp.float32, least / len(shards), high / len(shards))
        gain = gain * jnp.repeat(jnp.exp(steps), shape[dim] // shards_of).reshape((-1,) + (1,) * (len(shape) - 1 - dim))
    return gain


def shared_out(key, own, number, rows, number_of, top, bound, skew):
    order = jax.random.permutation(key, number_of)
    packed, ordinary = shares(number_of, rows * top, bound, skew, True), shares(number_of, rows * top, bound, skew, False)
    places = jnp.arange(number_of)

    def named(tallies, rotation):
        used = int((tallies > 0).sum())
        fixed = max(1, used // 4)
        passed = fixed + (places - fixed + rotation * (used - fixed)) % max(1, number_of - fixed)
        return jnp.zeros((number_of,), jnp.int32).at[order[jnp.where(places < fixed, places, passed)]].set(jnp.asarray(tallies, jnp.int32))

    tallies = jnp.where(number % 4 == 0, named(packed, number // 4), named(ordinary, number - number // 4 - 1))
    mixed = jax.random.permutation(jax.random.fold_in(own, 3), number_of)
    source_of, receiver = mixed[0:number_of // 2 * 2:2], mixed[1:number_of // 2 * 2:2]
    slack = jnp.minimum(tallies[source_of] - 1, bound - tallies[receiver]) // 2
    slack = jnp.where((source_of == order[0]) | (receiver == order[0]) | (tallies[receiver] == 0), 0, jnp.maximum(slack, 0))
    passed = jax.random.randint(jax.random.fold_in(own, 4), (number_of // 2,), 0, 1 << 20) % (slack + 1)
    tallies = tallies.at[source_of].add(-passed).at[receiver].add(passed)
    members = jnp.searchsorted(jnp.cumsum(tallies), jnp.arange(rows * top), side="right").astype(jnp.int32)
    grid = members.reshape(top, rows).T
    grid = grid[jax.random.permutation(jax.random.fold_in(own, 1), rows)]
    rotation = jax.random.randint(jax.random.fold_in(own, 2), (rows, 1), 0, top)
    return jnp.take_along_axis(grid, (jnp.arange(top)[None, :] + rotation) % top, axis=1)


def shares(amount, total, bound, lean, full):
    portions = [(1 << 20) // math.isqrt(standing ** lean) + 1 for standing in range(1, amount + 1)]
    largest = bound if full else min(bound, max(-(-total // amount), total * portions[0] // sum(portions)))
    least = 1 if total - largest >= amount - 1 else 0
    holding, surplus = [largest] + [least] * (amount - 1), total - largest - least * (amount - 1)
    while surplus > 0:
        free = [i for i in range(1, amount) if holding[i] < largest] or [i for i in range(1, amount) if holding[i] < bound]
        pool, remaining = sum([portions[i] for i in free]), surplus
        for i in free:
            addition = min(bound - holding[i], max(1, remaining * portions[i] // pool), surplus)
            holding[i] = holding[i] + addition
            surplus = surplus - addition
    return np.array(holding)


def scatter_about(key, extent, deviation, limit, pieces=(), held_as=jnp.bfloat16):
    result = jax.random.normal(key, extent, jnp.float32) * deviation
    if len(pieces) > 0:
        result = block_scale(key, extent, pieces, -0.22, 0.18) * result
    return jnp.clip(result, min=-limit, max=limit).astype(held_as)


def setup_inputs(seed: int = 0) -> dict:
    splits = jax.random.split(jax.random.key(seed), 6)
    coefficients = jnp.clip(2.0 * jax.random.uniform(splits[0], (TOKENS, ACTIVE, BLOCK), jnp.float32) ** block_scale(splits[0], (TOKENS, ACTIVE, BLOCK), ((0, 256),), -0.2, 0.2), 0.0, 2.0).astype(jnp.bfloat16)
    block_ids_keys = jax.random.split(jax.random.fold_in(splits[1], 1), TOKENS // TOK_LAT)
    block_ids_turns = jax.random.permutation(jax.random.fold_in(splits[1], 3), TOKENS // TOK_LAT)
    block_ids = jax.vmap(lambda own, number: shared_out(jax.random.fold_in(splits[1], 2), own, number, TOK_LAT, BLOCKS, ACTIVE, MOST, 2))(block_ids_keys, block_ids_turns).reshape((TOKENS, ACTIVE))
    counts = set_ends(jax.random.randint(splits[2], (TOKENS,), ACTIVE - ACTIVE * 3 // 8, ACTIVE + 1), jax.random.fold_in(splits[2], 1), ACTIVE - ACTIVE * 3 // 8, ACTIVE).astype(jnp.int32)
    decoder = scatter_about(splits[3], (LAYERS, LATENTS, D), (ACTIVE * BLOCK) ** -0.5, 0.125, ((1, 64), (2, 4)))
    bias = scatter_about(splits[4], (LAYERS, D), 0.5, 3.0, ((1, 4),), jnp.float32)
    return dict(coefficients=coefficients, block_ids=block_ids, counts=counts, decoder=decoder, bias=bias)


def slot_ranks(identity_row):
    length_total = identity_row.shape[0]
    serial = jnp.arange(length_total, dtype=jnp.int32)
    matches = (identity_row[:, None] == identity_row[None, :]) & (serial[None, :] < serial[:, None])
    return jnp.sum(matches.astype(jnp.int32), axis=1).astype(jnp.int32)


def reference(coefficients, block_ids, counts, decoder, bias):
    token_total = coefficients.shape[0]
    is_live = jnp.arange(ACTIVE, dtype=jnp.int32)[None, :] < counts[:, None]
    active_coeffs = jnp.where(is_live[:, :, None], coefficients, jnp.zeros((), coefficients.dtype))
    grouped = block_ids.reshape(N_LAT, TOK_LAT * ACTIVE)
    ranked = lax.map(slot_ranks, grouped)
    capacity = N_LAT * MOST
    sources = jnp.arange(N_LAT, dtype=jnp.int32)[:, None]
    position = (grouped * capacity + sources * MOST + ranked).reshape(-1).astype(jnp.int32)
    buffer = jnp.zeros((BLOCKS * capacity, BLOCK), coefficients.dtype).at[position].set(active_coeffs.reshape(-1, BLOCK))
    token_of = jnp.arange(token_total * ACTIVE, dtype=jnp.int32) // ACTIVE
    owners = jnp.zeros((BLOCKS * capacity,), jnp.int32).at[position].set(token_of)
    buffer = buffer.reshape(BLOCKS, capacity, BLOCK)
    owners = owners.reshape(BLOCKS, capacity)
    weights = decoder.reshape(LAYERS, BLOCKS, BLOCK, D)
    stride_blocks = math.gcd(BLOCKS, 16)

    def accumulate(summed, block_index):
        first_block = (block_index * stride_blocks).astype(jnp.int32)
        piece = lax.dynamic_slice_in_dim(buffer, first_block, stride_blocks, 0).astype(jnp.float32)
        weight_piece = lax.dynamic_slice_in_dim(weights, first_block, stride_blocks, 1).astype(jnp.float32)
        slot_rows = jnp.einsum("bmk,lbkd->lbmd", piece, weight_piece)
        targets = lax.dynamic_slice_in_dim(owners, first_block, stride_blocks, 0).reshape(-1)
        return summed.at[:, targets, :].add(slot_rows.reshape(LAYERS, -1, D)), None

    start_total = jnp.zeros((LAYERS, token_total, D), jnp.float32)
    summed, _ = lax.scan(accumulate, start_total, jnp.arange(BLOCKS // stride_blocks, dtype=jnp.int32))
    return (summed + bias[:, None, :]).astype(jnp.bfloat16)
```

```python
import functools

import jax
import jax.numpy as jnp
from jax import lax
from jax.experimental import pallas as pl
from jax.experimental.pallas import tpu as pltpu
from jax.sharding import Mesh
from jax.sharding import PartitionSpec as P

BLOCK = 128
MOST = 2
NZ, NY, NC, NX = 8, 4, 2, 4
N_LAT = NZ * NY * NC
TOK = 32
OWN = 8
ACTIVE = 16
BLOCKS_DEV = 16
SLOTS = BLOCKS_DEV * MOST
ROWS = SLOTS + 8
CHUNK = 16
CHUNKS = TOK // CHUNK
LIMIT = 32700.0
FLOOR = 2.0**-104
STEP = 256.0
LN2 = 0.6931471805599453

VMEM = pl.BlockSpec(memory_space=pltpu.VMEM)
ANY = pl.BlockSpec(memory_space=pl.ANY)
SMEM = pl.BlockSpec(memory_space=pltpu.SMEM)


def ring(n, k):
    return [(i, (i + k) % n) for i in range(n)]


def column(row):
    return jnp.transpose(jnp.broadcast_to(row, (128, 128)))


def pack_kernel(x_ref, part0, part1, part2, part3, out_ref):
    parts = (part0, part1, part2, part3)
    n_part = OWN * ACTIVE
    ids = []
    for part in parts:
        meta = part[n_part : n_part + 8, :].astype(jnp.float32)
        ids.append(meta[0:1, :] * 32.0 + meta[1:2, :])
    ids_lane = jnp.concatenate(ids, axis=1)
    total = n_part * NX
    count = jnp.zeros((1, total), jnp.float32)
    lane = lax.broadcasted_iota(jnp.int32, (n_part, total), 1)
    sub = lax.broadcasted_iota(jnp.int32, (n_part, total), 0)
    for r in range(NX):
        col = column(ids[r])
        same = jnp.concatenate([col] * NX, axis=1) == ids_lane
        before = sub + r * n_part < lane
        count = count + jnp.sum(jnp.where(same & before, 1.0, 0.0), axis=0, keepdims=True)
    pos = ids_lane * float(MOST) + count
    dst = jnp.floor(pos * (1.0 / SLOTS))
    slot = pos - dst * SLOTS
    dst_row = lax.broadcasted_iota(jnp.int32, (N_LAT, n_part), 0).astype(jnp.float32)
    slot_lane = lax.broadcasted_iota(jnp.int32, (n_part, 128), 1).astype(jnp.float32)
    token = lax.broadcasted_iota(jnp.int32, (n_part, 128), 0) // ACTIVE
    meta = jnp.zeros((N_LAT, 128), jnp.float32)
    for r in range(NX):
        here = slice(r * n_part, (r + 1) * n_part)
        pick = jnp.where(dst[:, here] == dst_row, 1.0, 0.0).astype(jnp.bfloat16)
        first = lax.rem(x_ref[0] - r + NX, NX) * OWN + 1
        named = (token + first).astype(jnp.float32)
        put = jnp.where(column(slot[:, here]) == slot_lane, named, 0.0).astype(jnp.bfloat16)
        meta = meta + jnp.dot(pick, put, preferred_element_type=jnp.float32)
    group = 8
    row = lax.broadcasted_iota(jnp.int32, (group * SLOTS, n_part), 0)
    for g in range(N_LAT // group):
        acc = jnp.zeros((group * SLOTS, BLOCK), jnp.float32)
        at = (row + g * group * SLOTS).astype(jnp.float32)
        for r in range(NX):
            here = slice(r * n_part, (r + 1) * n_part)
            hot = jnp.where(pos[:, here] == at, 1.0, 0.0).astype(jnp.bfloat16)
            acc = acc + jnp.dot(hot, parts[r][0:n_part, :], preferred_element_type=jnp.float32)
        acc = acc.astype(jnp.bfloat16)
        for k in range(group):
            d = g * group + k
            out_ref[d, 0:SLOTS, :] = acc[k * SLOTS : (k + 1) * SLOTS, :]
            out_ref[d, SLOTS:ROWS, :] = jnp.broadcast_to(meta[d : d + 1, :], (8, 128)).astype(
                jnp.bfloat16
            )


def quantized(acc):
    top = jnp.max(jnp.abs(acc), axis=1, keepdims=True)
    top = jnp.maximum(top, FLOOR) * (1.0 / LIMIT)
    code = jnp.ceil(jnp.log(top) * (STEP / LN2))
    scale = jnp.exp(code * (-LN2 / STEP))
    q = jnp.clip(jnp.floor(acc * scale + 0.5), -32767.0, 32767.0)
    return q.astype(jnp.int32).astype(jnp.int16), code


def expand_kernel(
    first, c_ref, own, other, w_own, w_other, out_ref, x_buf, w_buf, tok_buf, coef_buf, sems
):
    depth = w_other.shape[0]
    width = w_other.shape[1]
    at = pl.multiple_of(c_ref[0] * width, 128)
    copies = [
        pltpu.make_async_copy(w_own.at[0, :, pl.ds(at, width)], w_buf.at[0:depth], sems.at[0]),
        pltpu.make_async_copy(w_other, w_buf.at[depth : 2 * depth], sems.at[1]),
    ]
    for copy in copies:
        copy.start()
    for h, ref in enumerate((own, other)):
        meta = jnp.concatenate(
            [ref[s, SLOTS:ROWS, :].astype(jnp.float32)[0:1, :] for s in range(N_LAT)]
            + [jnp.zeros((128 - N_LAT, 128), jnp.float32)],
            axis=0,
        )
        turned = jnp.transpose(meta)
        for s in range(N_LAT):
            tok_buf[s, h * SLOTS : (h + 1) * SLOTS, :] = jnp.broadcast_to(
                turned[0:SLOTS, s : s + 1], (SLOTS, 128)
            )
            coef_buf[s, h * SLOTS : (h + 1) * SLOTS, :] = ref[s, 0:SLOTS, :].astype(jnp.float32)
    t = lax.broadcasted_iota(jnp.int32, (CHUNK, 128), 0).astype(jnp.float32) + float(first + 1)

    def build(s, carry):
        z = s // (NY * NC)
        y = (s // NC) % NY
        c = s % NC
        base = pl.multiple_of(((y * NZ + z) * NC + c) * CHUNK, CHUNK)
        for b in range(2 * BLOCKS_DEV):
            row = jnp.zeros((CHUNK, 128), jnp.float32)
            for m in range(MOST):
                k = b * MOST + m
                hit = jnp.broadcast_to(tok_buf[s, k : k + 1, :], (CHUNK, 128)) == t
                row = jnp.where(
                    hit, jnp.broadcast_to(coef_buf[s, k : k + 1, :], (CHUNK, 128)), row
                )
            x_buf[pl.ds(base, CHUNK), b * BLOCK : (b + 1) * BLOCK] = row.astype(jnp.bfloat16)
        return carry

    lax.fori_loop(0, N_LAT, build, 0)
    for copy in copies:
        copy.wait()
    part = NZ * NC * CHUNK
    for y in range(NY):
        acc = jnp.dot(
            x_buf[y * part : (y + 1) * part, :], w_buf[...], preferred_element_type=jnp.float32
        )
        q, code = quantized(acc)
        out_ref[y, 0:part, :] = q
        for k in range(part // 128):
            lanes = jnp.transpose(jnp.broadcast_to(code[k * 128 : (k + 1) * 128, :], (128, 128)))
            out_ref[y, part : part + 8, k * 128 : (k + 1) * 128] = (
                lanes[0:8, :].astype(jnp.int32).astype(jnp.int16)
            )


def middle_kernel(in_ref, out_ref):
    part = NZ * NC * CHUNK
    width = in_ref.shape[2]
    for k in range(part // 128):
        acc = jnp.zeros((128, width), jnp.float32)
        for y in range(NY):
            code = in_ref[y, part : part + 8, k * 128 : (k + 1) * 128]
            code = code.astype(jnp.int32).astype(jnp.float32)[0:1, :]
            scale = jnp.exp(column(code) * (LN2 / STEP))[:, 0:1]
            q = in_ref[y, k * 128 : (k + 1) * 128, :].astype(jnp.int32).astype(jnp.float32)
            acc = acc + q * scale
        q, code = quantized(acc)
        code = jnp.broadcast_to(code, (128, 128)).astype(jnp.int32).astype(jnp.int16)
        for j in range(128 // CHUNK):
            d = k * (128 // CHUNK) + j
            out_ref[d, :, 0:width] = q[j * CHUNK : (j + 1) * CHUNK, :]
            out_ref[d, :, width : width + 128] = code[j * CHUNK : (j + 1) * CHUNK, :]


def final_kernel(*refs):
    ins, bias, out_ref = refs[:CHUNKS], refs[CHUNKS], refs[CHUNKS + 1]
    width = out_ref.shape[2] // NC
    for k, ref in enumerate(ins):
        for c in range(NC):
            acc = jnp.broadcast_to(bias[:, c * width : (c + 1) * width], (CHUNK, width))
            for z in range(NZ):
                both = ref[z * NC + c].astype(jnp.int32).astype(jnp.float32)
                scale = jnp.exp(both[:, width : width + 1] * (LN2 / STEP))
                acc = acc + both[:, 0:width] * scale
            out_ref[0, k * CHUNK : (k + 1) * CHUNK, c * width : (c + 1) * width] = acc.astype(
                jnp.bfloat16
            )


def shards(coefficients, block_ids, counts, decoder, bias):
    core = lax.axis_index("c").astype(jnp.int32)
    x = lax.axis_index("x").astype(jnp.int32)
    depth, full = decoder.shape[1], decoder.shape[2]
    width = full // NC
    sent = lax.dynamic_slice(decoder[0], (0, (1 - core) * width), (depth, width))
    w_other = lax.ppermute(sent, "c", ring(NC, 1))

    live = lax.broadcasted_iota(jnp.int32, (OWN, ACTIVE), 1) < counts[:, None]
    coeffs = jnp.where(live[:, :, None], coefficients, jnp.zeros((), coefficients.dtype))
    flat = block_ids.reshape(1, OWN * ACTIVE)
    packed = jnp.concatenate(
        [
            coeffs.reshape(OWN * ACTIVE, BLOCK),
            (flat // 32).astype(jnp.bfloat16),
            (flat % 32).astype(jnp.bfloat16),
            jnp.zeros((6, BLOCK), jnp.bfloat16),
        ],
        axis=0,
    )
    parts = [packed] + [lax.ppermute(packed, "x", ring(NX, k)) for k in range(1, NX)]
    outgoing = pl.pallas_call(
        pack_kernel,
        out_shape=jax.ShapeDtypeStruct((N_LAT, ROWS, BLOCK), jnp.bfloat16),
        in_specs=[SMEM] + [VMEM] * NX,
        out_specs=VMEM,
        name="pack",
    )(x.reshape(1), *parts)
    own = lax.all_to_all(outgoing, ("z", "y", "c"), 0, 0, tiled=True)
    other = lax.ppermute(own, "c", ring(NC, 1))

    part = NZ * NC * CHUNK
    arrived = []
    for q in range(CHUNKS):
        sums = pl.pallas_call(
            functools.partial(expand_kernel, q * CHUNK),
            out_shape=jax.ShapeDtypeStruct((NY, part + 8, width), jnp.int16),
            in_specs=[SMEM, VMEM, VMEM, ANY, ANY],
            out_specs=VMEM,
            scratch_shapes=[
                pltpu.VMEM((NY * part, 2 * depth), jnp.bfloat16),
                pltpu.VMEM((2 * depth, width), jnp.bfloat16),
                pltpu.VMEM((N_LAT, 2 * SLOTS, BLOCK), jnp.float32),
                pltpu.VMEM((N_LAT, 2 * SLOTS, BLOCK), jnp.float32),
                pltpu.SemaphoreType.DMA((2,)),
            ],
            compiler_params=pltpu.CompilerParams(vmem_limit_bytes=40 * 1024 * 1024),
            cost_estimate=pl.CostEstimate(
                flops=2 * NY * part * 2 * depth * width,
                bytes_accessed=8 * 1024 * 1024,
                transcendentals=0,
            ),
            name=f"expand{q}",
        )(core.reshape(1), own, other, decoder, w_other)
        crossed = lax.all_to_all(sums, "y", 0, 0, tiled=True)
        halfway = pl.pallas_call(
            middle_kernel,
            out_shape=jax.ShapeDtypeStruct((NZ * NC, CHUNK, width + 128), jnp.int16),
            in_specs=[VMEM],
            out_specs=VMEM,
            name=f"middle{q}",
        )(crossed)
        arrived.append(lax.all_to_all(halfway, ("z", "c"), 0, 0, tiled=True))
    return pl.pallas_call(
        final_kernel,
        out_shape=jax.ShapeDtypeStruct((1, TOK, full), jnp.bfloat16),
        in_specs=[VMEM] * (CHUNKS + 1),
        out_specs=VMEM,
        name="final",
    )(*arrived, bias)


def solution(mesh):
    split = Mesh(mesh.devices.reshape(NZ, NY, NC, NX), ("z", "y", "c", "x"))
    lat = ("z", "y", "c")
    in_specs = (
        P((*lat, "x"), None, None),
        P((*lat, "x"), None),
        P((*lat, "x")),
        P(None, lat, "x"),
        P(None, "x"),
    )
    return jax.shard_map(
        shards, mesh=split, in_specs=in_specs, out_specs=P(None, lat, "x"), check_vma=False
    )
```

```python
import functools

import jax
import jax.numpy as jnp
from jax import lax
from jax.experimental import pallas as pl
from jax.experimental.pallas import tpu as pltpu
from jax.sharding import Mesh
from jax.sharding import PartitionSpec as P


BLOCK = 128
MOST = 2
NZ, NY, NC, NX = 8, 4, 2, 4
CHIPS = NZ * NY
TOK = 32
OWN = 8
ACTIVE = 16
BLOCKS_DEV = 16
BLOCKS_CHIP = BLOCKS_DEV * NC
HALF = BLOCKS_DEV * MOST
SLOTS = BLOCKS_CHIP * MOST
ROWS = SLOTS + 8
CHUNK = 16
CHUNKS = TOK // CHUNK
PART = NZ // 2 * NC * CHUNK
LIMIT = 32700.0
FLOOR = 2.0**-104
STEP = 256.0
LN2 = 0.6931471805599453
MIB = 1024 * 1024

VMEM = pl.BlockSpec(memory_space=pltpu.VMEM)
SMEM = pl.BlockSpec(memory_space=pltpu.SMEM)
HBM = pl.BlockSpec(memory_space=pltpu.HBM)
ANY = pl.BlockSpec(memory_space=pl.ANY)
PIECES = 2
GRANT = 48


def ring(n, k):
    return [(i, (i + k) % n) for i in range(n)]


def call(kernel, out_shape, in_specs, mib, flops=0, scratch=()):
    return pl.pallas_call(
        kernel,
        out_shape=out_shape,
        in_specs=in_specs,
        out_specs=jax.tree.map(lambda _: VMEM, out_shape),
        scratch_shapes=list(scratch),
        compiler_params=pltpu.CompilerParams(vmem_limit_bytes=mib * MIB),
        cost_estimate=pl.CostEstimate(flops=flops, bytes_accessed=2 * MIB, transcendentals=0),
    )


def column(row):
    return jnp.transpose(jnp.broadcast_to(row, (128, 128)))


def pack_kernel(info, part0, part1, part2, part3, out_ref):
    parts = (part0, part1, part2, part3)
    n_part = OWN * ACTIVE
    ids = []
    for part in parts:
        meta = part[n_part : n_part + 8, :].astype(jnp.float32)
        ids.append(meta[0:1, :] * 32.0 + meta[1:2, :])
    ids_lane = jnp.concatenate(ids, axis=1)
    total = n_part * NX
    count = jnp.zeros((1, total), jnp.float32)
    lane = lax.broadcasted_iota(jnp.int32, (n_part, total), 1)
    sub = lax.broadcasted_iota(jnp.int32, (n_part, total), 0)
    for r in range(NX):
        col = column(ids[r])
        same = jnp.concatenate([col] * NX, axis=1) == ids_lane
        before = sub + r * n_part < lane
        count = count + jnp.sum(jnp.where(same & before, 1.0, 0.0), axis=0, keepdims=True)
    pos = ids_lane * float(MOST) + count
    dst = jnp.floor(pos * (1.0 / SLOTS))
    slot = pos - dst * SLOTS
    dst_row = lax.broadcasted_iota(jnp.int32, (CHIPS, n_part), 0).astype(jnp.float32)
    slot_lane = lax.broadcasted_iota(jnp.int32, (n_part, 128), 1).astype(jnp.float32)
    token = lax.broadcasted_iota(jnp.int32, (n_part, 128), 0) // ACTIVE
    meta = jnp.zeros((CHIPS, 128), jnp.float32)
    for r in range(NX):
        here = slice(r * n_part, (r + 1) * n_part)
        pick = jnp.where(dst[:, here] == dst_row, 1.0, 0.0).astype(jnp.bfloat16)
        first = lax.rem(info[0] - r + NX, NX) * OWN + 1
        named = (token + first).astype(jnp.float32)
        put = jnp.where(column(slot[:, here]) == slot_lane, named, 0.0).astype(jnp.bfloat16)
        meta = meta + jnp.dot(pick, put, preferred_element_type=jnp.float32)
    group = 4
    row = lax.broadcasted_iota(jnp.int32, (group * SLOTS, n_part), 0)
    for g in range(CHIPS // group):
        acc = jnp.zeros((group * SLOTS, BLOCK), jnp.float32)
        at = (row + g * group * SLOTS).astype(jnp.float32)
        for r in range(NX):
            here = slice(r * n_part, (r + 1) * n_part)
            hot = jnp.where(pos[:, here] == at, 1.0, 0.0).astype(jnp.bfloat16)
            acc = acc + jnp.dot(hot, parts[r][0:n_part, :], preferred_element_type=jnp.float32)
        acc = acc.astype(jnp.bfloat16)
        for k in range(group):
            d = g * group + k
            out_ref[d, 0:SLOTS, :] = acc[k * SLOTS : (k + 1) * SLOTS, :]
            out_ref[d, SLOTS:ROWS, :] = jnp.broadcast_to(meta[d : d + 1, :], (8, 128)).astype(
                jnp.bfloat16
            )


def prepare_kernel(info, own, other, tok_ref, coef_ref):
    core = info[0]
    sources = (own, other)
    meta = jnp.concatenate(
        [
            ref[s, SLOTS:ROWS, :].astype(jnp.float32)[0:1, :]
            for ref in sources
            for s in range(CHIPS)
        ]
        + [jnp.zeros((128 - 2 * CHIPS, 128), jnp.float32)],
        axis=0,
    )
    turned = jnp.transpose(meta)
    for n in range(2 * CHIPS):
        ref, s = sources[n // CHIPS], n % CHIPS
        for h in range(NC):
            to = pl.ds(pl.multiple_of(lax.rem(core + h, NC) * HALF, HALF), HALF)
            here = slice(h * HALF, (h + 1) * HALF)
            tok_ref[n, to, :] = jnp.broadcast_to(turned[here, n : n + 1], (HALF, 128))
            coef_ref[n, to, :] = ref[s, here, :].astype(jnp.float32)


def quantized(acc):
    top = jnp.max(jnp.abs(acc), axis=1, keepdims=True)
    top = jnp.maximum(top, FLOOR) * (1.0 / LIMIT)
    code = jnp.ceil(jnp.log(top) * (STEP / LN2))
    scale = jnp.exp(code * (-LN2 / STEP))
    q = jnp.clip(jnp.floor(acc * scale + 0.5), -32767.0, 32767.0)
    return q.astype(jnp.int32).astype(jnp.int16), code


def write_message(out_ref, acc):
    n = acc.shape[0]
    q, code = quantized(acc)
    out_ref[0:n, :] = q
    for k in range(n // 128):
        lanes = jnp.transpose(jnp.broadcast_to(code[k * 128 : (k + 1) * 128, :], (128, 128)))
        out_ref[n : n + 8, k * 128 : (k + 1) * 128] = (
            lanes[0:8, :].astype(jnp.int32).astype(jnp.int16)
        )


def read_message(ref, k):
    n = ref.shape[0] - 8
    code = ref[n : n + 8, k * 128 : (k + 1) * 128]
    code = code.astype(jnp.int32).astype(jnp.float32)[0:1, :]
    scale = jnp.exp(column(code) * (LN2 / STEP))[:, 0:1]
    return ref[k * 128 : (k + 1) * 128, :].astype(jnp.int32).astype(jnp.float32) * scale


def expand_kernel(first, send, info, tok, coef, w_own, w_other, after, *rest):
    outs, (x_buf, w_buf, acc, sems) = rest[:-4], rest[-4:]
    depth = w_own.shape[1]
    width = w_buf.shape[1]
    core = info[0]
    columns = pl.ds(pl.multiple_of(core * width, 128), width)
    deep = depth // PIECES
    copies = []
    for g in range(NC * PIECES):
        ref = (w_own, w_other)[g // PIECES]
        k = g % PIECES
        copies.append(
            pltpu.make_async_copy(
                ref.at[0, k * deep : (k + 1) * deep, columns],
                w_buf.at[g * deep : (g + 1) * deep],
                sems.at[g],
            )
        )
    for copy in copies:
        copy.start()
    t = lax.broadcasted_iota(jnp.int32, (CHUNK, 128), 0).astype(jnp.float32) + float(first + 1)
    blocks = BLOCKS_CHIP // (NC * PIECES)
    for g, copy in enumerate(copies):

        def build(i, carry, g=g):
            h, j, z, c = i // 16, (i // 8) % 2, (i // 2) % 4, i % 2
            n = lax.rem(c + core, NC) * CHIPS + (h * 4 + z) * NY + info[1 + h * 2 + j]
            base = pl.multiple_of(i * CHUNK, CHUNK)
            for b in range(g * blocks, (g + 1) * blocks):
                row = jnp.zeros((CHUNK, 128), jnp.float32)
                for m in range(MOST):
                    k = b * MOST + m
                    hit = jnp.broadcast_to(tok[n, k : k + 1, :], (CHUNK, 128)) == t
                    row = jnp.where(
                        hit, jnp.broadcast_to(coef[n, k : k + 1, :], (CHUNK, 128)), row
                    )
                x_buf[pl.ds(base, CHUNK), b * BLOCK : (b + 1) * BLOCK] = row.astype(jnp.bfloat16)
            return carry

        lax.fori_loop(0, 4 * PART // CHUNK, build, 0)
        copy.wait()
        here = slice(g * deep, (g + 1) * deep)
        term = jnp.dot(x_buf[:, here], w_buf[here, :], preferred_element_type=jnp.float32)
        if g == 0:
            acc[...] = term
        elif send or g < NC * PIECES - 1:
            acc[...] += term
        else:
            outs[0][...] = acc[...] + term
    if send:
        for h in range(2):
            write_message(outs[h], acc[h * 2 * PART : (h + 1) * 2 * PART, :])


def middle_kernel(kept, in0, in1, after, keep_ref, out0, out1):
    for h, (ref, out) in enumerate(((in0, out0), (in1, out1))):
        keep_ref[h * PART : (h + 1) * PART, :] = kept[
            2 * h * PART : (2 * h + 1) * PART, :
        ] + read_message(ref, 0)
        write_message(
            out, kept[(2 * h + 1) * PART : (2 * h + 2) * PART, :] + read_message(ref, 1)
        )


def last_kernel(*refs):
    ins, out_ref = refs[:-1], refs[-1]
    width = ins[0].shape[1]
    for q in range(CHUNKS):
        kept, messages = ins[3 * q], ins[3 * q + 1 : 3 * q + 3]
        for h, ref in enumerate(messages):
            acc = kept[h * PART : (h + 1) * PART, :] + read_message(ref, 0)
            v, code = quantized(acc)
            code = jnp.broadcast_to(code, (PART, 128)).astype(jnp.int32).astype(jnp.int16)
            for j in range(PART // CHUNK):
                d = h * (PART // CHUNK) + j
                at, here = slice(q * CHUNK, (q + 1) * CHUNK), slice(j * CHUNK, (j + 1) * CHUNK)
                out_ref[d, at, 0:width] = v[here, :]
                out_ref[d, at, width : width + 128] = code[here, :]


def final_kernel(ref, bias, out_ref):
    width = out_ref.shape[2] // NC
    for c in range(NC):
        acc = jnp.broadcast_to(bias[:, c * width : (c + 1) * width], (TOK, width))
        for z in range(NZ):
            both = ref[z * NC + c].astype(jnp.int32).astype(jnp.float32)
            scale = jnp.exp(both[:, width : width + 1] * (LN2 / STEP))
            acc = acc + both[:, 0:width] * scale
        out_ref[0, :, c * width : (c + 1) * width] = acc.astype(jnp.bfloat16)


def run(coefficients, block_ids, counts, decoder, bias):
    core = lax.axis_index("c").astype(jnp.int32)
    x = lax.axis_index("x").astype(jnp.int32)
    y = lax.axis_index("y").astype(jnp.int32)
    depth, full = decoder.shape[1], decoder.shape[2]
    width = full // NC
    w_other = lax.ppermute(decoder, "c", ring(NC, 1))

    live = lax.broadcasted_iota(jnp.int32, (OWN, ACTIVE), 1) < counts[:, None]
    coeffs = jnp.where(live[:, :, None], coefficients, jnp.zeros((), coefficients.dtype))
    flat = block_ids.reshape(1, OWN * ACTIVE)
    packed = jnp.concatenate(
        [
            coeffs.reshape(OWN * ACTIVE, BLOCK),
            (flat // 32).astype(jnp.bfloat16),
            (flat % 32).astype(jnp.bfloat16),
            jnp.zeros((6, BLOCK), jnp.bfloat16),
        ],
        axis=0,
    )
    parts = [packed] + [lax.ppermute(packed, "x", ring(NX, k)) for k in range(1, NX)]
    shape = jax.ShapeDtypeStruct
    outgoing = call(
        pack_kernel, shape((CHIPS, ROWS, BLOCK), jnp.bfloat16), [SMEM] + [VMEM] * NX, 10
    )(x.reshape(1), *parts)
    own = lax.all_to_all(outgoing, ("z", "y"), 0, 0, tiled=True)
    other = lax.ppermute(own, "c", ring(NC, 1))
    slots = shape((2 * CHIPS, SLOTS, BLOCK), jnp.float32)
    tok, coef = call(prepare_kernel, [slots, slots], [SMEM, VMEM, VMEM], 10)(
        core.reshape(1), own, other
    )

    pair_a, pair_b = [(i, i ^ 1) for i in range(NY)], [(i, NY - 1 - i) for i in range(NY)]
    a, b = y ^ 1, NY - 1 - y
    opposite = NY - 1 - a
    sent_to = jnp.stack([core, a, opposite, b, opposite])
    kept_for = jnp.stack([core, y, b, y, a])
    message = shape((2 * PART + 8, width), jnp.int16)
    small = shape((PART + 8, width), jnp.int16)

    def expand(q, send, after):
        return call(
            functools.partial(expand_kernel, q * CHUNK, send),
            [message, message] if send else [shape((4 * PART, width), jnp.float32)],
            [SMEM, VMEM, VMEM, HBM, HBM, ANY],
            GRANT,
            flops=2 * 4 * PART * 2 * depth * width,
            scratch=[
                pltpu.VMEM((4 * PART, 2 * depth), jnp.bfloat16),
                pltpu.VMEM((2 * depth, width), jnp.bfloat16),
                pltpu.VMEM((4 * PART, width), jnp.float32),
                pltpu.SemaphoreType.DMA((NC * PIECES,)),
            ],
        )(sent_to if send else kept_for, tok, coef, decoder, w_other, after)

    after = own
    crossing = []
    for q in range(CHUNKS):
        m0, m1 = expand(q, True, after)
        after = m0
        crossing.append((lax.ppermute(m0, "y", pair_a), lax.ppermute(m1, "y", pair_b)))
    arrived = []
    for q in range(CHUNKS):
        (kept,) = expand(q, False, after)
        kept, m0, m1 = call(
            middle_kernel,
            [shape((2 * PART, width), jnp.float32), small, small],
            [VMEM] * 3 + [ANY],
            10,
        )(kept, *crossing[q], after)
        after = m0
        m0 = lax.ppermute(m0, "y", pair_b)
        m1 = lax.ppermute(m1, "y", pair_a)
        arrived += [kept, m0, m1]
    out = call(
        last_kernel, shape((NZ * NC, TOK, width + 128), jnp.int16), [VMEM] * 3 * CHUNKS, 10
    )(*arrived)
    return call(
        final_kernel, shape((1, TOK, full), jnp.bfloat16), [VMEM] * 2, 10
    )(lax.all_to_all(out, ("z", "c"), 0, 0, tiled=True), bias)


def solution(mesh):
    split = Mesh(mesh.devices.reshape(NZ, NY, NC, NX), ("z", "y", "c", "x"))
    lat = ("z", "y", "c")
    in_specs = (
        P((*lat, "x"), None, None),
        P((*lat, "x"), None),
        P((*lat, "x")),
        P(None, lat, "x"),
        P(None, "x"),
    )
    return jax.shard_map(
        run, mesh=split, in_specs=in_specs, out_specs=P(None, lat, "x"), check_vma=False
    )
```

```python
import functools

import jax
import jax.numpy as jnp
from jax import lax
from jax.experimental import pallas as pl
from jax.experimental.pallas import tpu as pltpu
from jax.sharding import Mesh
from jax.sharding import PartitionSpec as P


BLOCK = 128
MOST = 2
NZ, NY, NC, NX = 8, 4, 2, 4
CHIPS = NZ * NY
TOK = 32
OWN = 8
ACTIVE = 16
BLOCKS_DEV = 16
BLOCKS_CHIP = BLOCKS_DEV * NC
HALF = BLOCKS_DEV * MOST
SLOTS = BLOCKS_CHIP * MOST
ROWS = SLOTS + 8
CHUNK = 16
CHUNKS = TOK // CHUNK
PART = NZ // 2 * NC * CHUNK
LIMIT = 32700.0
FLOOR = 2.0**-104
STEP = 256.0
LN2 = 0.6931471805599453
MIB = 1024 * 1024

VMEM = pl.BlockSpec(memory_space=pltpu.VMEM)
SMEM = pl.BlockSpec(memory_space=pltpu.SMEM)
HBM = pl.BlockSpec(memory_space=pltpu.HBM)
ANY = pl.BlockSpec(memory_space=pl.ANY)
PIECES = 2
GRANT = 24
WEIGHT_GRANT = 8


def ring(n, k):
    return [(i, (i + k) % n) for i in range(n)]


def call(kernel, out_shape, in_specs, mib, flops=0, scratch=()):
    return pl.pallas_call(
        kernel,
        out_shape=out_shape,
        in_specs=in_specs,
        out_specs=jax.tree.map(lambda _: VMEM, out_shape),
        scratch_shapes=list(scratch),
        compiler_params=pltpu.CompilerParams(vmem_limit_bytes=mib * MIB),
        cost_estimate=pl.CostEstimate(flops=flops, bytes_accessed=2 * MIB, transcendentals=0),
    )


def column(row):
    return jnp.transpose(jnp.broadcast_to(row, (128, 128)))


def pack_kernel(info, part0, part1, part2, part3, out_ref):
    parts = (part0, part1, part2, part3)
    n_part = OWN * ACTIVE
    ids = []
    for part in parts:
        meta = part[n_part : n_part + 8, :].astype(jnp.float32)
        ids.append(meta[0:1, :] * 32.0 + meta[1:2, :])
    ids_lane = jnp.concatenate(ids, axis=1)
    total = n_part * NX
    count = jnp.zeros((1, total), jnp.float32)
    lane = lax.broadcasted_iota(jnp.int32, (n_part, total), 1)
    sub = lax.broadcasted_iota(jnp.int32, (n_part, total), 0)
    for r in range(NX):
        col = column(ids[r])
        same = jnp.concatenate([col] * NX, axis=1) == ids_lane
        before = sub + r * n_part < lane
        count = count + jnp.sum(jnp.where(same & before, 1.0, 0.0), axis=0, keepdims=True)
    pos = ids_lane * float(MOST) + count
    dst = jnp.floor(pos * (1.0 / SLOTS))
    slot = pos - dst * SLOTS
    dst_row = lax.broadcasted_iota(jnp.int32, (CHIPS, n_part), 0).astype(jnp.float32)
    slot_lane = lax.broadcasted_iota(jnp.int32, (n_part, 128), 1).astype(jnp.float32)
    token = lax.broadcasted_iota(jnp.int32, (n_part, 128), 0) // ACTIVE
    meta = jnp.zeros((CHIPS, 128), jnp.float32)
    for r in range(NX):
        here = slice(r * n_part, (r + 1) * n_part)
        pick = jnp.where(dst[:, here] == dst_row, 1.0, 0.0).astype(jnp.bfloat16)
        first = lax.rem(info[0] - r + NX, NX) * OWN + 1
        named = (token + first).astype(jnp.float32)
        put = jnp.where(column(slot[:, here]) == slot_lane, named, 0.0).astype(jnp.bfloat16)
        meta = meta + jnp.dot(pick, put, preferred_element_type=jnp.float32)
    group = 4
    row = lax.broadcasted_iota(jnp.int32, (group * SLOTS, n_part), 0)
    for g in range(CHIPS // group):
        acc = jnp.zeros((group * SLOTS, BLOCK), jnp.float32)
        at = (row + g * group * SLOTS).astype(jnp.float32)
        for r in range(NX):
            here = slice(r * n_part, (r + 1) * n_part)
            hot = jnp.where(pos[:, here] == at, 1.0, 0.0).astype(jnp.bfloat16)
            acc = acc + jnp.dot(hot, parts[r][0:n_part, :], preferred_element_type=jnp.float32)
        acc = acc.astype(jnp.bfloat16)
        for k in range(group):
            d = g * group + k
            out_ref[d, 0:SLOTS, :] = acc[k * SLOTS : (k + 1) * SLOTS, :]
            out_ref[d, SLOTS:ROWS, :] = jnp.broadcast_to(meta[d : d + 1, :], (8, 128)).astype(
                jnp.bfloat16
            )


def prepare_kernel(info, own, other, tok_ref, coef_ref):
    core = info[0]
    sources = (own, other)
    meta = jnp.concatenate(
        [
            ref[s, SLOTS:ROWS, :].astype(jnp.float32)[0:1, :]
            for ref in sources
            for s in range(CHIPS)
        ]
        + [jnp.zeros((128 - 2 * CHIPS, 128), jnp.float32)],
        axis=0,
    )
    turned = jnp.transpose(meta)
    for n in range(2 * CHIPS):
        ref, s = sources[n // CHIPS], n % CHIPS
        for h in range(NC):
            to = pl.ds(pl.multiple_of(lax.rem(core + h, NC) * HALF, HALF), HALF)
            here = slice(h * HALF, (h + 1) * HALF)
            tok_ref[n, to, :] = jnp.broadcast_to(turned[here, n : n + 1], (HALF, 128))
            coef_ref[n, to, :] = ref[s, here, :].astype(jnp.float32)


def quantized(acc):
    top = jnp.max(jnp.abs(acc), axis=1, keepdims=True)
    top = jnp.maximum(top, FLOOR) * (1.0 / LIMIT)
    code = jnp.ceil(jnp.log(top) * (STEP / LN2))
    scale = jnp.exp(code * (-LN2 / STEP))
    q = jnp.clip(jnp.floor(acc * scale + 0.5), -32767.0, 32767.0)
    return q.astype(jnp.int32).astype(jnp.int16), code


def write_message(out_ref, acc):
    n = acc.shape[0]
    q, code = quantized(acc)
    out_ref[0:n, :] = q
    for k in range(n // 128):
        lanes = jnp.transpose(jnp.broadcast_to(code[k * 128 : (k + 1) * 128, :], (128, 128)))
        out_ref[n : n + 8, k * 128 : (k + 1) * 128] = (
            lanes[0:8, :].astype(jnp.int32).astype(jnp.int16)
        )


def read_message(ref, k):
    n = ref.shape[0] - 8
    code = ref[n : n + 8, k * 128 : (k + 1) * 128]
    code = code.astype(jnp.int32).astype(jnp.float32)[0:1, :]
    scale = jnp.exp(column(code) * (LN2 / STEP))[:, 0:1]
    return ref[k * 128 : (k + 1) * 128, :].astype(jnp.int32).astype(jnp.float32) * scale


def weights_kernel(core_ref, w_own, w_other, after, out_ref, sems):
    depth, width = w_own.shape[1], out_ref.shape[1]
    columns = pl.ds(pl.multiple_of(core_ref[0] * width, 128), width)
    deep = depth // PIECES
    copies = []
    for g in range(NC * PIECES):
        ref = (w_own, w_other)[g // PIECES]
        k = g % PIECES
        copies.append(
            pltpu.make_async_copy(
                ref.at[0, k * deep : (k + 1) * deep, columns],
                out_ref.at[g * deep : (g + 1) * deep],
                sems.at[g],
            )
        )
    for copy in copies:
        copy.start()
    for copy in copies:
        copy.wait()


def expand_kernel(first, send, info, tok, coef, weights, after, *rest):
    outs, x_buf = rest[:-1], rest[-1]
    core = info[0]
    t = lax.broadcasted_iota(jnp.int32, (CHUNK, 128), 0).astype(jnp.float32) + float(first + 1)

    def build(i, carry):
        h, j, z, c = i // 16, (i // 8) % 2, (i // 2) % 4, i % 2
        n = lax.rem(c + core, NC) * CHIPS + (h * 4 + z) * NY + info[1 + h * 2 + j]
        base = pl.multiple_of(i * CHUNK, CHUNK)
        for b in range(BLOCKS_CHIP):
            row = jnp.zeros((CHUNK, 128), jnp.float32)
            for m in range(MOST):
                k = b * MOST + m
                hit = jnp.broadcast_to(tok[n, k : k + 1, :], (CHUNK, 128)) == t
                row = jnp.where(
                    hit, jnp.broadcast_to(coef[n, k : k + 1, :], (CHUNK, 128)), row
                )
            x_buf[pl.ds(base, CHUNK), b * BLOCK : (b + 1) * BLOCK] = row.astype(jnp.bfloat16)
        return carry

    lax.fori_loop(0, 4 * PART // CHUNK, build, 0)
    for h in range(2):
        here = slice(h * 2 * PART, (h + 1) * 2 * PART)
        acc = jnp.dot(x_buf[here, :], weights[...], preferred_element_type=jnp.float32)
        if send:
            write_message(outs[h], acc)
        else:
            outs[0][here, :] = acc


def middle_kernel(kept, in0, in1, after, keep_ref, out0, out1):
    for h, (ref, out) in enumerate(((in0, out0), (in1, out1))):
        keep_ref[h * PART : (h + 1) * PART, :] = kept[
            2 * h * PART : (2 * h + 1) * PART, :
        ] + read_message(ref, 0)
        write_message(
            out, kept[(2 * h + 1) * PART : (2 * h + 2) * PART, :] + read_message(ref, 1)
        )


def last_kernel(*refs):
    ins, out_ref = refs[:-1], refs[-1]
    width = ins[0].shape[1]
    for q in range(CHUNKS):
        kept, messages = ins[3 * q], ins[3 * q + 1 : 3 * q + 3]
        for h, ref in enumerate(messages):
            acc = kept[h * PART : (h + 1) * PART, :] + read_message(ref, 0)
            v, code = quantized(acc)
            code = jnp.broadcast_to(code, (PART, 128)).astype(jnp.int32).astype(jnp.int16)
            for j in range(PART // CHUNK):
                d = h * (PART // CHUNK) + j
                at, here = slice(q * CHUNK, (q + 1) * CHUNK), slice(j * CHUNK, (j + 1) * CHUNK)
                out_ref[d, at, 0:width] = v[here, :]
                out_ref[d, at, width : width + 128] = code[here, :]


def final_kernel(ref, bias, out_ref):
    width = out_ref.shape[2] // NC
    for c in range(NC):
        acc = jnp.broadcast_to(bias[:, c * width : (c + 1) * width], (TOK, width))
        for z in range(NZ):
            both = ref[z * NC + c].astype(jnp.int32).astype(jnp.float32)
            scale = jnp.exp(both[:, width : width + 1] * (LN2 / STEP))
            acc = acc + both[:, 0:width] * scale
        out_ref[0, :, c * width : (c + 1) * width] = acc.astype(jnp.bfloat16)


def run(coefficients, block_ids, counts, decoder, bias):
    core = lax.axis_index("c").astype(jnp.int32)
    x = lax.axis_index("x").astype(jnp.int32)
    y = lax.axis_index("y").astype(jnp.int32)
    depth, full = decoder.shape[1], decoder.shape[2]
    width = full // NC
    w_other = lax.ppermute(decoder, "c", ring(NC, 1))

    live = lax.broadcasted_iota(jnp.int32, (OWN, ACTIVE), 1) < counts[:, None]
    coeffs = jnp.where(live[:, :, None], coefficients, jnp.zeros((), coefficients.dtype))
    flat = block_ids.reshape(1, OWN * ACTIVE)
    packed = jnp.concatenate(
        [
            coeffs.reshape(OWN * ACTIVE, BLOCK),
            (flat // 32).astype(jnp.bfloat16),
            (flat % 32).astype(jnp.bfloat16),
            jnp.zeros((6, BLOCK), jnp.bfloat16),
        ],
        axis=0,
    )
    parts = [packed] + [lax.ppermute(packed, "x", ring(NX, k)) for k in range(1, NX)]
    shape = jax.ShapeDtypeStruct
    outgoing = call(
        pack_kernel, shape((CHIPS, ROWS, BLOCK), jnp.bfloat16), [SMEM] + [VMEM] * NX, 10
    )(x.reshape(1), *parts)
    own = lax.all_to_all(outgoing, ("z", "y"), 0, 0, tiled=True)
    weights = call(
        weights_kernel,
        shape((NC * depth, width), jnp.bfloat16),
        [SMEM, HBM, HBM, ANY],
        WEIGHT_GRANT,
        flops=10**10,
        scratch=[pltpu.SemaphoreType.DMA((NC * PIECES,))],
    )(core.reshape(1), decoder, w_other, outgoing)
    other = lax.ppermute(own, "c", ring(NC, 1))
    slots = shape((2 * CHIPS, SLOTS, BLOCK), jnp.float32)
    tok, coef = call(prepare_kernel, [slots, slots], [SMEM, VMEM, VMEM], 10)(
        core.reshape(1), own, other
    )

    pair_a, pair_b = [(i, i ^ 1) for i in range(NY)], [(i, NY - 1 - i) for i in range(NY)]
    a, b = y ^ 1, NY - 1 - y
    opposite = NY - 1 - a
    sent_to = jnp.stack([core, a, opposite, b, opposite])
    kept_for = jnp.stack([core, y, b, y, a])
    message = shape((2 * PART + 8, width), jnp.int16)
    small = shape((PART + 8, width), jnp.int16)

    def expand(q, send, after):
        return call(
            functools.partial(expand_kernel, q * CHUNK, send),
            [message, message] if send else [shape((4 * PART, width), jnp.float32)],
            [SMEM, VMEM, VMEM, VMEM, ANY],
            GRANT,
            flops=2 * 4 * PART * 2 * depth * width,
            scratch=[pltpu.VMEM((4 * PART, 2 * depth), jnp.bfloat16)],
        )(sent_to if send else kept_for, tok, coef, weights, after)

    after = own
    crossing = []
    for q in range(CHUNKS):
        m0, m1 = expand(q, True, after)
        after = m0
        crossing.append((lax.ppermute(m0, "y", pair_a), lax.ppermute(m1, "y", pair_b)))
    arrived = []
    for q in range(CHUNKS):
        (kept,) = expand(q, False, after)
        kept, m0, m1 = call(
            middle_kernel,
            [shape((2 * PART, width), jnp.float32), small, small],
            [VMEM] * 3 + [ANY],
            10,
        )(kept, *crossing[q], after)
        after = m0
        m0 = lax.ppermute(m0, "y", pair_b)
        m1 = lax.ppermute(m1, "y", pair_a)
        arrived += [kept, m0, m1]
    out = call(
        last_kernel, shape((NZ * NC, TOK, width + 128), jnp.int16), [VMEM] * 3 * CHUNKS, 10
    )(*arrived)
    return call(
        final_kernel, shape((1, TOK, full), jnp.bfloat16), [VMEM] * 2, 10
    )(lax.all_to_all(out, ("z", "c"), 0, 0, tiled=True), bias)


def solution(mesh):
    split = Mesh(mesh.devices.reshape(NZ, NY, NC, NX), ("z", "y", "c", "x"))
    lat = ("z", "y", "c")
    in_specs = (
        P((*lat, "x"), None, None),
        P((*lat, "x"), None),
        P((*lat, "x")),
        P(None, lat, "x"),
        P(None, "x"),
    )
    return jax.shard_map(
        run, mesh=split, in_specs=in_specs, out_specs=P(None, lat, "x"), check_vma=False
    )
```

```python
import jax
import jax.numpy as jnp
from jax import lax
from jax.experimental import pallas as pl
from jax.experimental.pallas import tpu as pltpu
from jax.sharding import Mesh
from jax.sharding import PartitionSpec as P


BLOCK = 128
MOST = 2
NZ, NY, NC, NX = 8, 4, 2, 4
CHIPS = NZ * NY
TOK = 32
OWN = 8
ACTIVE = 16
BLOCKS_DEV = 16
BLOCKS_CHIP = BLOCKS_DEV * NC
HALF = BLOCKS_DEV * MOST
SLOTS = BLOCKS_CHIP * MOST
ROWS = SLOTS + 8
PART = NZ // 2 * TOK
LIMIT = 32700.0
FLOOR = 2.0**-104
STEP = 256.0
LN2 = 0.6931471805599453
MIB = 1024 * 1024

VMEM = pl.BlockSpec(memory_space=pltpu.VMEM)
SMEM = pl.BlockSpec(memory_space=pltpu.SMEM)
HBM = pl.BlockSpec(memory_space=pltpu.HBM)
ANY = pl.BlockSpec(memory_space=pl.ANY)
PIECES = 4
GRANT = 48
WEIGHT_GRANT = 50


def ring(n, k):
    return [(i, (i + k) % n) for i in range(n)]


def call(kernel, out_shape, in_specs, mib, flops=0, scratch=()):
    return pl.pallas_call(
        kernel,
        out_shape=out_shape,
        in_specs=in_specs,
        out_specs=jax.tree.map(lambda _: VMEM, out_shape),
        scratch_shapes=list(scratch),
        compiler_params=pltpu.CompilerParams(vmem_limit_bytes=mib * MIB),
        cost_estimate=pl.CostEstimate(flops=flops, bytes_accessed=2 * MIB, transcendentals=0),
    )


def column(row):
    return jnp.transpose(jnp.broadcast_to(row, (128, 128)))


def wrap_kernel(counts, coeffs, ids, out_ref):
    n = OWN * ACTIVE
    slot = lax.broadcasted_iota(jnp.int32, (ACTIVE, BLOCK), 0)
    for i in range(OWN):
        live = slot < counts[i]
        rows = jnp.where(live, coeffs[i].astype(jnp.float32), 0.0)
        out_ref[i * ACTIVE : (i + 1) * ACTIVE, :] = rows.astype(jnp.bfloat16)
    high = (ids[...] // 32).astype(jnp.float32)
    low = ids[...].astype(jnp.float32) - high * 32.0
    repeat = lax.broadcasted_iota(jnp.int32, (ACTIVE, n), 1) % ACTIVE
    repeat = jnp.where(repeat == lax.broadcasted_iota(jnp.int32, (ACTIVE, n), 0), 1.0, 0.0)
    token = lax.broadcasted_iota(jnp.int32, (OWN, n), 0)
    mine = lax.broadcasted_iota(jnp.int32, (OWN, n), 1) // ACTIVE == token
    meta = jnp.zeros((OWN, n), jnp.float32)
    for k, part in enumerate((high, low)):
        wide = jnp.dot(
            part.astype(jnp.bfloat16),
            repeat.astype(jnp.bfloat16),
            preferred_element_type=jnp.float32,
        )
        row = jnp.sum(jnp.where(mine, wide, 0.0), axis=0, keepdims=True)
        meta = jnp.where(token == k, jnp.broadcast_to(row, (OWN, n)), meta)
    out_ref[n : n + OWN, :] = meta.astype(jnp.bfloat16)


def pack_kernel(info, part0, part1, part2, part3, out_ref):
    parts = (part0, part1, part2, part3)
    n_part = OWN * ACTIVE
    ids = []
    for part in parts:
        meta = part[n_part : n_part + 8, :].astype(jnp.float32)
        ids.append(meta[0:1, :] * 32.0 + meta[1:2, :])
    ids_lane = jnp.concatenate(ids, axis=1)
    total = n_part * NX
    count = jnp.zeros((1, total), jnp.float32)
    lane = lax.broadcasted_iota(jnp.int32, (n_part, total), 1)
    sub = lax.broadcasted_iota(jnp.int32, (n_part, total), 0)
    for r in range(NX):
        col = column(ids[r])
        same = jnp.concatenate([col] * NX, axis=1) == ids_lane
        before = sub + r * n_part < lane
        count = count + jnp.sum(jnp.where(same & before, 1.0, 0.0), axis=0, keepdims=True)
    pos = ids_lane * float(MOST) + count
    dst = jnp.floor(pos * (1.0 / SLOTS))
    slot = pos - dst * SLOTS
    dst_row = lax.broadcasted_iota(jnp.int32, (CHIPS, n_part), 0).astype(jnp.float32)
    slot_lane = lax.broadcasted_iota(jnp.int32, (n_part, 128), 1).astype(jnp.float32)
    token = lax.broadcasted_iota(jnp.int32, (n_part, 128), 0) // ACTIVE
    meta = jnp.zeros((CHIPS, 128), jnp.float32)
    for r in range(NX):
        here = slice(r * n_part, (r + 1) * n_part)
        pick = jnp.where(dst[:, here] == dst_row, 1.0, 0.0).astype(jnp.bfloat16)
        first = lax.rem(info[0] - r + NX, NX) * OWN + 1
        named = (token + first).astype(jnp.float32)
        put = jnp.where(column(slot[:, here]) == slot_lane, named, 0.0).astype(jnp.bfloat16)
        meta = meta + jnp.dot(pick, put, preferred_element_type=jnp.float32)
    group = 4
    row = lax.broadcasted_iota(jnp.int32, (group * SLOTS, n_part), 0)
    for g in range(CHIPS // group):
        acc = jnp.zeros((group * SLOTS, BLOCK), jnp.float32)
        at = (row + g * group * SLOTS).astype(jnp.float32)
        for r in range(NX):
            here = slice(r * n_part, (r + 1) * n_part)
            hot = jnp.where(pos[:, here] == at, 1.0, 0.0).astype(jnp.bfloat16)
            acc = acc + jnp.dot(hot, parts[r][0:n_part, :], preferred_element_type=jnp.float32)
        acc = acc.astype(jnp.bfloat16)
        for k in range(group):
            d = g * group + k
            out_ref[d, 0:SLOTS, :] = acc[k * SLOTS : (k + 1) * SLOTS, :]
            out_ref[d, SLOTS:ROWS, :] = jnp.broadcast_to(meta[d : d + 1, :], (8, 128)).astype(
                jnp.bfloat16
            )


def prepare(info, arrived, tok_ref, coef_ref):
    core = info[0]
    meta = jnp.concatenate(
        [arrived[s, SLOTS:ROWS, :].astype(jnp.float32)[0:1, :] for s in range(CHIPS)]
        + [jnp.zeros((128 - CHIPS, 128), jnp.float32)],
        axis=0,
    )
    turned = jnp.transpose(meta)
    for s in range(CHIPS):
        for h in range(NC):
            to = pl.ds(pl.multiple_of(lax.rem(core + h, NC) * HALF, HALF), HALF)
            here = slice(h * HALF, (h + 1) * HALF)
            tok_ref[s, to, :] = jnp.broadcast_to(turned[here, s : s + 1], (HALF, 128))
            coef_ref[s, to, :] = arrived[s, here, :].astype(jnp.float32)


def quantized(acc):
    top = jnp.max(jnp.abs(acc), axis=1, keepdims=True)
    top = jnp.maximum(top, FLOOR) * (1.0 / LIMIT)
    code = jnp.ceil(jnp.log(top) * (STEP / LN2))
    scale = jnp.exp(code * (-LN2 / STEP))
    q = jnp.clip(jnp.floor(acc * scale + 0.5), -32767.0, 32767.0)
    return q.astype(jnp.int32).astype(jnp.int16), code


def write_message(out_ref, acc):
    n = acc.shape[0]
    q, code = quantized(acc)
    out_ref[0:n, :] = q
    for k in range(n // 128):
        lanes = jnp.transpose(jnp.broadcast_to(code[k * 128 : (k + 1) * 128, :], (128, 128)))
        out_ref[n : n + 8, k * 128 : (k + 1) * 128] = (
            lanes[0:8, :].astype(jnp.int32).astype(jnp.int16)
        )


def read_message(ref, k):
    n = ref.shape[0] - 8
    code = ref[n : n + 8, k * 128 : (k + 1) * 128]
    code = code.astype(jnp.int32).astype(jnp.float32)[0:1, :]
    scale = jnp.exp(column(code) * (LN2 / STEP))[:, 0:1]
    return ref[k * 128 : (k + 1) * 128, :].astype(jnp.int32).astype(jnp.float32) * scale


def weights_kernel(core_ref, w_own, w_other, after, out_ref, sems):
    depth, width = w_own.shape[1], out_ref.shape[1]
    columns = pl.ds(pl.multiple_of(core_ref[0] * width, 128), width)
    deep = NC * depth // PIECES
    copies = []
    for g in range(PIECES):
        ref = (w_own, w_other)[g // (PIECES // NC)]
        k = g % (PIECES // NC)
        copies.append(
            pltpu.make_async_copy(
                ref.at[0, k * deep : (k + 1) * deep, columns],
                out_ref.at[g * deep : (g + 1) * deep],
                sems.at[g],
            )
        )
    for copy in copies:
        copy.start()
    for copy in copies:
        copy.wait()


def build(info, tok, coef, x_buf):
    t = lax.broadcasted_iota(jnp.int32, (TOK, 128), 0).astype(jnp.float32) + 1.0

    def source(i, carry):
        h, j, z = i // 8, (i // 4) % 2, i % 4
        n = (h * 4 + z) * NY + info[1 + h * 2 + j]
        base = pl.multiple_of(i * TOK, TOK)
        for b in range(BLOCKS_CHIP):
            row = jnp.zeros((TOK, 128), jnp.float32)
            for m in range(MOST):
                k = b * MOST + m
                hit = jnp.broadcast_to(tok[n, k : k + 1, :], (TOK, 128)) == t
                row = jnp.where(hit, jnp.broadcast_to(coef[n, k : k + 1, :], (TOK, 128)), row)
            x_buf[pl.ds(base, TOK), b * BLOCK : (b + 1) * BLOCK] = row.astype(jnp.bfloat16)
        return carry

    lax.fori_loop(0, 4 * PART // TOK, source, 0)


def multiply(info, arrived, weights, tok, coef, x_buf, w_buf, sems, acc):
    deep = w_buf.shape[0] // PIECES
    copies = []
    for g in range(PIECES):
        here = slice(g * deep, (g + 1) * deep)
        copies.append(pltpu.make_async_copy(weights.at[here], w_buf.at[here], sems.at[g]))
    for copy in copies:
        copy.start()
    prepare(info, arrived, tok, coef)
    build(info, tok, coef, x_buf)
    for g, copy in enumerate(copies):
        here = slice(g * deep, (g + 1) * deep)
        copy.wait()
        term = jnp.dot(x_buf[:, here], w_buf[here, :], preferred_element_type=jnp.float32)
        acc[...] = term if g == 0 else acc[...] + term


def send_kernel(info, arrived, weights, after, out0, out1, acc, *scratch):
    multiply(info, arrived, weights, *scratch, acc)
    for h, out in enumerate((out0, out1)):
        write_message(out, acc[h * 2 * PART : (h + 1) * 2 * PART, :])


def keep_kernel(info, arrived, weights, after, out_ref, *scratch):
    multiply(info, arrived, weights, *scratch, out_ref)


def keep_middle_kernel(
    info, arrived, weights, after, in0, in1, keep_ref, out0, out1, acc, *scratch
):
    multiply(info, arrived, weights, *scratch, acc)
    for h, (ref, out) in enumerate(((in0, out0), (in1, out1))):
        low, high = 2 * h * PART, (2 * h + 1) * PART
        keep_ref[h * PART : (h + 1) * PART, :] = acc[low:high, :] + read_message(ref, 0)
        write_message(out, acc[high : high + PART, :] + read_message(ref, 1))


def middle_kernel(kept, in0, in1, keep_ref, out0, out1):
    for h, (ref, out) in enumerate(((in0, out0), (in1, out1))):
        keep_ref[h * PART : (h + 1) * PART, :] = kept[
            2 * h * PART : (2 * h + 1) * PART, :
        ] + read_message(ref, 0)
        write_message(
            out, kept[(2 * h + 1) * PART : (2 * h + 2) * PART, :] + read_message(ref, 1)
        )


def last_kernel(info, *refs):
    ins, out_ref = refs[:-1], refs[-1]
    width = ins[0].shape[1]
    for q in range(NC):
        kept, messages = ins[3 * q], ins[3 * q + 1 : 3 * q + 3]
        c = lax.rem(info[0] + q, NC)
        for h, ref in enumerate(messages):
            acc = kept[h * PART : (h + 1) * PART, :] + read_message(ref, 0)
            v, code = quantized(acc)
            code = jnp.broadcast_to(code, (PART, 128)).astype(jnp.int32).astype(jnp.int16)
            for j in range(PART // TOK):
                d = (h * (PART // TOK) + j) * NC + c
                here = slice(j * TOK, (j + 1) * TOK)
                out_ref[d, :, 0:width] = v[here, :]
                out_ref[d, :, width : width + 128] = code[here, :]


def final_kernel(ref, bias, out_ref):
    width = out_ref.shape[2] // NC
    for c in range(NC):
        acc = jnp.broadcast_to(bias[:, c * width : (c + 1) * width], (TOK, width))
        for z in range(NZ):
            both = ref[z * NC + c].astype(jnp.int32).astype(jnp.float32)
            scale = jnp.exp(both[:, width : width + 1] * (LN2 / STEP))
            acc = acc + both[:, 0:width] * scale
        out_ref[0, :, c * width : (c + 1) * width] = acc.astype(jnp.bfloat16)


def run(coefficients, block_ids, counts, decoder, bias):
    core = lax.axis_index("c").astype(jnp.int32)
    x = lax.axis_index("x").astype(jnp.int32)
    y = lax.axis_index("y").astype(jnp.int32)
    depth, full = decoder.shape[1], decoder.shape[2]
    width = full // NC
    w_other = lax.ppermute(decoder, "c", ring(NC, 1))

    shape = jax.ShapeDtypeStruct
    packed = call(
        wrap_kernel, shape((OWN * (ACTIVE + 1), BLOCK), jnp.bfloat16), [SMEM, VMEM, VMEM], 10
    )(counts, coefficients, block_ids)
    parts = [packed] + [lax.ppermute(packed, "x", ring(NX, k)) for k in range(1, NX)]
    outgoing = call(
        pack_kernel, shape((CHIPS, ROWS, BLOCK), jnp.bfloat16), [SMEM] + [VMEM] * NX, 10
    )(x.reshape(1), *parts)
    own = lax.all_to_all(outgoing, ("z", "y"), 0, 0, tiled=True)
    weights = call(
        weights_kernel,
        shape((NC * depth, width), jnp.bfloat16),
        [SMEM, HBM, HBM, ANY],
        WEIGHT_GRANT,
        flops=10**10,
        scratch=[pltpu.SemaphoreType.DMA((PIECES,))],
    )(core.reshape(1), decoder, w_other, outgoing)
    other = lax.ppermute(own, "c", ring(NC, 1))
    pair_a, pair_b = [(i, i ^ 1) for i in range(NY)], [(i, NY - 1 - i) for i in range(NY)]
    a, b = y ^ 1, NY - 1 - y
    opposite = NY - 1 - a
    sent_to = jnp.stack([core, a, opposite, b, opposite])
    kept_for = jnp.stack([core, y, b, y, a])
    message = shape((2 * PART + 8, width), jnp.int16)
    small = shape((PART + 8, width), jnp.int16)

    kept = shape((2 * PART, width), jnp.float32)
    product = {"flops": 2 * 4 * PART * NC * depth * width}
    total = pltpu.VMEM((4 * PART, width), jnp.float32)
    scratch = [
        pltpu.VMEM((CHIPS, SLOTS, BLOCK), jnp.float32),
        pltpu.VMEM((CHIPS, SLOTS, BLOCK), jnp.float32),
        pltpu.VMEM((4 * PART, NC * depth), jnp.bfloat16),
        pltpu.VMEM((NC * depth, width), jnp.bfloat16),
        pltpu.SemaphoreType.DMA((PIECES,)),
    ]
    given = [SMEM, VMEM, HBM, ANY]

    def cross(m0, m1, pair0, pair1):
        m0 = lax.ppermute(m0, "y", pair0)
        m1 = lax.ppermute(m1, "y", pair1)
        return m0, m1

    m0, m1 = call(
        send_kernel, [message, message], given, GRANT, scratch=[total] + scratch, **product
    )(sent_to, own, weights, own)
    crossing0 = cross(m0, m1, pair_a, pair_b)
    m0, m1 = call(
        send_kernel, [message, message], given, GRANT, scratch=[total] + scratch, **product
    )(sent_to, other, weights, m0)
    crossing1 = cross(m0, m1, pair_a, pair_b)
    (sums,) = call(
        keep_kernel,
        [shape((4 * PART, width), jnp.float32)],
        given,
        GRANT,
        scratch=scratch,
        **product,
    )(kept_for, own, weights, m0)
    kept0, m0, m1 = call(middle_kernel, [kept, small, small], [VMEM] * 3, 10)(sums, *crossing0)
    arrived0 = cross(m0, m1, pair_b, pair_a)
    kept1, m0, m1 = call(
        keep_middle_kernel,
        [kept, small, small],
        given + [VMEM] * 2,
        GRANT,
        scratch=[total] + scratch,
        **product,
    )(kept_for, other, weights, m0, *crossing1)
    arrived1 = cross(m0, m1, pair_b, pair_a)
    out = call(
        last_kernel, shape((NZ * NC, TOK, width + 128), jnp.int16), [SMEM] + [VMEM] * 6, 10
    )(core.reshape(1), kept0, *arrived0, kept1, *arrived1)
    return call(
        final_kernel, shape((1, TOK, full), jnp.bfloat16), [VMEM] * 2, 10
    )(lax.all_to_all(out, ("z", "c"), 0, 0, tiled=True), bias)


def solution(mesh):
    split = Mesh(mesh.devices.reshape(NZ, NY, NC, NX), ("z", "y", "c", "x"))
    lat = ("z", "y", "c")
    in_specs = (
        P((*lat, "x"), None, None),
        P((*lat, "x"), None),
        P((*lat, "x")),
        P(None, lat, "x"),
        P(None, "x"),
    )
    return jax.shard_map(
        run, mesh=split, in_specs=in_specs, out_specs=P(None, lat, "x"), check_vma=False
    )
```

```python
import jax
import jax.numpy as jnp
from jax import lax
from jax.experimental import pallas as pl
from jax.experimental.pallas import tpu as pltpu
from jax.sharding import Mesh
from jax.sharding import PartitionSpec as P


BLOCK = 128
MOST = 2
NZ, NY, NC, NX = 8, 4, 2, 4
CHIPS = NZ * NY
TOK = 32
OWN = 8
ACTIVE = 16
BLOCKS_DEV = 16
BLOCKS_CHIP = BLOCKS_DEV * NC
HALF = BLOCKS_DEV * MOST
SLOTS = BLOCKS_CHIP * MOST
ROWS = SLOTS + 8
PART = NZ // 2 * TOK
LIMIT = 32700.0
FLOOR = 2.0**-104
STEP = 256.0
LN2 = 0.6931471805599453
MIB = 1024 * 1024

VMEM = pl.BlockSpec(memory_space=pltpu.VMEM)
SMEM = pl.BlockSpec(memory_space=pltpu.SMEM)
HBM = pl.BlockSpec(memory_space=pltpu.HBM)
ANY = pl.BlockSpec(memory_space=pl.ANY)
PIECES = 4
GRANT = 18
WEIGHT_GRANT = 8


def ring(n, k):
    return [(i, (i + k) % n) for i in range(n)]


def call(kernel, out_shape, in_specs, mib, flops=0, scratch=()):
    return pl.pallas_call(
        kernel,
        out_shape=out_shape,
        in_specs=in_specs,
        out_specs=jax.tree.map(lambda _: VMEM, out_shape),
        scratch_shapes=list(scratch),
        compiler_params=pltpu.CompilerParams(vmem_limit_bytes=mib * MIB),
        cost_estimate=pl.CostEstimate(flops=flops, bytes_accessed=2 * MIB, transcendentals=0),
    )


def column(row):
    return jnp.transpose(jnp.broadcast_to(row, (128, 128)))


def wrap_kernel(counts_in, coeffs_in, ids_in, out_ref, counts, coeffs, ids, sems):
    n = OWN * ACTIVE
    copies = [
        pltpu.make_async_copy(ref, to, sems.at[k])
        for k, (ref, to) in enumerate(
            ((counts_in, counts), (coeffs_in, coeffs), (ids_in, ids))
        )
    ]
    for copy in copies:
        copy.start()
    for copy in copies:
        copy.wait()
    slot = lax.broadcasted_iota(jnp.int32, (ACTIVE, BLOCK), 0)
    for i in range(OWN):
        live = slot < counts[i]
        rows = jnp.where(live, coeffs[i].astype(jnp.float32), 0.0)
        out_ref[i * ACTIVE : (i + 1) * ACTIVE, :] = rows.astype(jnp.bfloat16)
    high = (ids[...] // 32).astype(jnp.float32)
    low = ids[...].astype(jnp.float32) - high * 32.0
    repeat = lax.broadcasted_iota(jnp.int32, (ACTIVE, n), 1) % ACTIVE
    repeat = jnp.where(repeat == lax.broadcasted_iota(jnp.int32, (ACTIVE, n), 0), 1.0, 0.0)
    token = lax.broadcasted_iota(jnp.int32, (OWN, n), 0)
    mine = lax.broadcasted_iota(jnp.int32, (OWN, n), 1) // ACTIVE == token
    meta = jnp.zeros((OWN, n), jnp.float32)
    for k, part in enumerate((high, low)):
        wide = jnp.dot(
            part.astype(jnp.bfloat16),
            repeat.astype(jnp.bfloat16),
            preferred_element_type=jnp.float32,
        )
        row = jnp.sum(jnp.where(mine, wide, 0.0), axis=0, keepdims=True)
        meta = jnp.where(token == k, jnp.broadcast_to(row, (OWN, n)), meta)
    out_ref[n : n + OWN, :] = meta.astype(jnp.bfloat16)


def pack_kernel(info, part0, part1, part2, part3, out_ref):
    parts = (part0, part1, part2, part3)
    n_part = OWN * ACTIVE
    ids = []
    for part in parts:
        meta = part[n_part : n_part + 8, :].astype(jnp.float32)
        ids.append(meta[0:1, :] * 32.0 + meta[1:2, :])
    ids_lane = jnp.concatenate(ids, axis=1)
    total = n_part * NX
    count = jnp.zeros((1, total), jnp.float32)
    lane = lax.broadcasted_iota(jnp.int32, (n_part, total), 1)
    sub = lax.broadcasted_iota(jnp.int32, (n_part, total), 0)
    for r in range(NX):
        col = column(ids[r])
        same = jnp.concatenate([col] * NX, axis=1) == ids_lane
        before = sub + r * n_part < lane
        count = count + jnp.sum(jnp.where(same & before, 1.0, 0.0), axis=0, keepdims=True)
    pos = ids_lane * float(MOST) + count
    dst = jnp.floor(pos * (1.0 / SLOTS))
    slot = pos - dst * SLOTS
    dst_row = lax.broadcasted_iota(jnp.int32, (CHIPS, n_part), 0).astype(jnp.float32)
    slot_lane = lax.broadcasted_iota(jnp.int32, (n_part, 128), 1).astype(jnp.float32)
    token = lax.broadcasted_iota(jnp.int32, (n_part, 128), 0) // ACTIVE
    meta = jnp.zeros((CHIPS, 128), jnp.float32)
    for r in range(NX):
        here = slice(r * n_part, (r + 1) * n_part)
        pick = jnp.where(dst[:, here] == dst_row, 1.0, 0.0).astype(jnp.bfloat16)
        first = lax.rem(info[0] - r + NX, NX) * OWN + 1
        named = (token + first).astype(jnp.float32)
        put = jnp.where(column(slot[:, here]) == slot_lane, named, 0.0).astype(jnp.bfloat16)
        meta = meta + jnp.dot(pick, put, preferred_element_type=jnp.float32)
    group = 4
    row = lax.broadcasted_iota(jnp.int32, (group * SLOTS, n_part), 0)
    for g in range(CHIPS // group):
        acc = jnp.zeros((group * SLOTS, BLOCK), jnp.float32)
        at = (row + g * group * SLOTS).astype(jnp.float32)
        for r in range(NX):
            here = slice(r * n_part, (r + 1) * n_part)
            hot = jnp.where(pos[:, here] == at, 1.0, 0.0).astype(jnp.bfloat16)
            acc = acc + jnp.dot(hot, parts[r][0:n_part, :], preferred_element_type=jnp.float32)
        acc = acc.astype(jnp.bfloat16)
        for k in range(group):
            d = g * group + k
            out_ref[d, 0:SLOTS, :] = acc[k * SLOTS : (k + 1) * SLOTS, :]
            out_ref[d, SLOTS:ROWS, :] = jnp.broadcast_to(meta[d : d + 1, :], (8, 128)).astype(
                jnp.bfloat16
            )


def prepare(info, arrived, tok_ref, coef_ref):
    core = info[0]
    meta = jnp.concatenate(
        [arrived[s, SLOTS:ROWS, :].astype(jnp.float32)[0:1, :] for s in range(CHIPS)]
        + [jnp.zeros((128 - CHIPS, 128), jnp.float32)],
        axis=0,
    )
    turned = jnp.transpose(meta)
    for s in range(CHIPS):
        for h in range(NC):
            to = pl.ds(pl.multiple_of(lax.rem(core + h, NC) * HALF, HALF), HALF)
            here = slice(h * HALF, (h + 1) * HALF)
            tok_ref[s, to, :] = jnp.broadcast_to(turned[here, s : s + 1], (HALF, 128))
            coef_ref[s, to, :] = arrived[s, here, :].astype(jnp.float32)


def quantized(acc):
    top = jnp.max(jnp.abs(acc), axis=1, keepdims=True)
    top = jnp.maximum(top, FLOOR) * (1.0 / LIMIT)
    code = jnp.ceil(jnp.log(top) * (STEP / LN2))
    scale = jnp.exp(code * (-LN2 / STEP))
    q = jnp.clip(jnp.floor(acc * scale + 0.5), -32767.0, 32767.0)
    return q.astype(jnp.int32).astype(jnp.int16), code


def write_message(out_ref, acc):
    n = acc.shape[0]
    q, code = quantized(acc)
    out_ref[0:n, :] = q
    for k in range(n // 128):
        lanes = jnp.transpose(jnp.broadcast_to(code[k * 128 : (k + 1) * 128, :], (128, 128)))
        out_ref[n : n + 8, k * 128 : (k + 1) * 128] = (
            lanes[0:8, :].astype(jnp.int32).astype(jnp.int16)
        )


def read_message(ref, k):
    n = ref.shape[0] - 8
    code = ref[n : n + 8, k * 128 : (k + 1) * 128]
    code = code.astype(jnp.int32).astype(jnp.float32)[0:1, :]
    scale = jnp.exp(column(code) * (LN2 / STEP))[:, 0:1]
    return ref[k * 128 : (k + 1) * 128, :].astype(jnp.int32).astype(jnp.float32) * scale


def weights_kernel(core_ref, w_own, w_other, after, out_ref, sems):
    depth, width = w_own.shape[1], out_ref.shape[1]
    columns = pl.ds(pl.multiple_of(core_ref[0] * width, 128), width)
    deep = NC * depth // PIECES
    copies = []
    for g in range(PIECES):
        ref = (w_own, w_other)[g // (PIECES // NC)]
        k = g % (PIECES // NC)
        copies.append(
            pltpu.make_async_copy(
                ref.at[0, k * deep : (k + 1) * deep, columns],
                out_ref.at[g * deep : (g + 1) * deep],
                sems.at[g],
            )
        )
    for copy in copies:
        copy.start()
    for copy in copies:
        copy.wait()


def build(info, tok, coef, x_buf):
    t = lax.broadcasted_iota(jnp.int32, (TOK, 128), 0).astype(jnp.float32) + 1.0

    def source(i, carry):
        h, j, z = i // 8, (i // 4) % 2, i % 4
        n = (h * 4 + z) * NY + info[1 + h * 2 + j]
        base = pl.multiple_of(i * TOK, TOK)
        for b in range(BLOCKS_CHIP):
            row = jnp.zeros((TOK, 128), jnp.float32)
            for m in range(MOST):
                k = b * MOST + m
                hit = jnp.broadcast_to(tok[n, k : k + 1, :], (TOK, 128)) == t
                row = jnp.where(hit, jnp.broadcast_to(coef[n, k : k + 1, :], (TOK, 128)), row)
            x_buf[pl.ds(base, TOK), b * BLOCK : (b + 1) * BLOCK] = row.astype(jnp.bfloat16)
        return carry

    lax.fori_loop(0, 4 * PART // TOK, source, 0)


def multiply(info, arrived, weights, tok, coef, x_buf, acc):
    prepare(info, arrived, tok, coef)
    build(info, tok, coef, x_buf)
    for h in range(2):
        here = slice(h * 2 * PART, (h + 1) * 2 * PART)
        acc[here, :] = jnp.dot(
            x_buf[here, :], weights[...], preferred_element_type=jnp.float32
        )


def send_kernel(info, arrived, weights, after, out0, out1, acc, *scratch):
    multiply(info, arrived, weights, *scratch, acc)
    for h, out in enumerate((out0, out1)):
        write_message(out, acc[h * 2 * PART : (h + 1) * 2 * PART, :])


def keep_kernel(info, arrived, weights, after, out_ref, *scratch):
    multiply(info, arrived, weights, *scratch, out_ref)


def keep_middle_kernel(
    info, arrived, weights, after, in0, in1, keep_ref, out0, out1, acc, *scratch
):
    multiply(info, arrived, weights, *scratch, acc)
    for h, (ref, out) in enumerate(((in0, out0), (in1, out1))):
        low, high = 2 * h * PART, (2 * h + 1) * PART
        keep_ref[h * PART : (h + 1) * PART, :] = acc[low:high, :] + read_message(ref, 0)
        write_message(out, acc[high : high + PART, :] + read_message(ref, 1))


def middle_kernel(kept, in0, in1, keep_ref, out0, out1):
    for h, (ref, out) in enumerate(((in0, out0), (in1, out1))):
        keep_ref[h * PART : (h + 1) * PART, :] = kept[
            2 * h * PART : (2 * h + 1) * PART, :
        ] + read_message(ref, 0)
        write_message(
            out, kept[(2 * h + 1) * PART : (2 * h + 2) * PART, :] + read_message(ref, 1)
        )


def last_kernel(info, kept, in0, in1, *rest):
    outs, acc = rest[:-1], rest[-1]
    width = kept.shape[1]
    for h, ref in enumerate((in0, in1)):
        here = slice(h * PART, (h + 1) * PART)
        acc[here, :] = kept[here, :] + read_message(ref, 0)
    for k, out in enumerate(outs):
        rows = pl.ds(pl.multiple_of(lax.rem(info[1] + k, NZ) * TOK, TOK), TOK)
        if out.shape[1] == width:
            out[...] = acc[rows, :]
            continue
        v, code = quantized(acc[rows, :])
        out[:, 0:width] = v
        code = jnp.broadcast_to(code, (TOK, 128)).astype(jnp.int32).astype(jnp.int16)
        out[:, width : width + 128] = code


def final_kernel(info, bias, kept, *refs):
    ins, out_ref = refs[:-1], refs[-1]
    width = kept.shape[1]
    acc = kept[...]
    for q in range(NC):
        if q > 0:
            acc = jnp.zeros_like(acc)
        for ref in ins[0 : NZ - 1] if q == 0 else ins[NZ - 1 :]:
            both = ref[...].astype(jnp.int32).astype(jnp.float32)
            scale = jnp.exp(both[:, width : width + 1] * (LN2 / STEP))
            acc = acc + both[:, 0:width] * scale
        at = pl.ds(pl.multiple_of(lax.rem(info[0] + q, NC) * width, 128), width)
        out_ref[0, :, at] = (acc + bias[:, at]).astype(jnp.bfloat16)


def run(coefficients, block_ids, counts, decoder, bias):
    core = lax.axis_index("c").astype(jnp.int32)
    x = lax.axis_index("x").astype(jnp.int32)
    y = lax.axis_index("y").astype(jnp.int32)
    depth, full = decoder.shape[1], decoder.shape[2]
    width = full // NC
    w_other = lax.ppermute(decoder, "c", ring(NC, 1))

    shape = jax.ShapeDtypeStruct
    packed = call(
        wrap_kernel,
        shape((OWN * (ACTIVE + 1), BLOCK), jnp.bfloat16),
        [HBM, HBM, HBM],
        10,
        scratch=[
            pltpu.SMEM((OWN,), jnp.int32),
            pltpu.VMEM((OWN, ACTIVE, BLOCK), jnp.bfloat16),
            pltpu.VMEM((OWN, ACTIVE), jnp.int32),
            pltpu.SemaphoreType.DMA((3,)),
        ],
    )(counts, coefficients, block_ids)
    parts = [packed] + [lax.ppermute(packed, "x", ring(NX, k)) for k in range(1, NX)]
    outgoing = call(
        pack_kernel, shape((CHIPS, ROWS, BLOCK), jnp.bfloat16), [SMEM] + [VMEM] * NX, 10
    )(x.reshape(1), *parts)
    own = lax.all_to_all(outgoing, ("z", "y"), 0, 0, tiled=True)
    weights = call(
        weights_kernel,
        shape((NC * depth, width), jnp.bfloat16),
        [SMEM, HBM, HBM, ANY],
        WEIGHT_GRANT,
        flops=10**10,
        scratch=[pltpu.SemaphoreType.DMA((PIECES,))],
    )(core.reshape(1), decoder, w_other, outgoing)
    other = lax.ppermute(own, "c", ring(NC, 1))
    pair_a, pair_b = [(i, i ^ 1) for i in range(NY)], [(i, NY - 1 - i) for i in range(NY)]
    a, b = y ^ 1, NY - 1 - y
    opposite = NY - 1 - a
    sent_to = jnp.stack([core, a, opposite, b, opposite])
    kept_for = jnp.stack([core, y, b, y, a])
    message = shape((2 * PART + 8, width), jnp.int16)
    small = shape((PART + 8, width), jnp.int16)

    kept = shape((2 * PART, width), jnp.float32)
    product = {"flops": 2 * 4 * PART * NC * depth * width}
    total = pltpu.VMEM((4 * PART, width), jnp.float32)
    scratch = [
        pltpu.VMEM((CHIPS, SLOTS, BLOCK), jnp.float32),
        pltpu.VMEM((CHIPS, SLOTS, BLOCK), jnp.float32),
        pltpu.VMEM((4 * PART, NC * depth), jnp.bfloat16),
    ]
    given = [SMEM, VMEM, VMEM, ANY]

    def cross(m0, m1, pair0, pair1):
        m0 = lax.ppermute(m0, "y", pair0)
        m1 = lax.ppermute(m1, "y", pair1)
        return m0, m1

    m0, m1 = call(
        send_kernel, [message, message], given, GRANT, scratch=[total] + scratch, **product
    )(sent_to, own, weights, own)
    crossing0 = cross(m0, m1, pair_a, pair_b)
    m0, m1 = call(
        send_kernel, [message, message], given, GRANT, scratch=[total] + scratch, **product
    )(sent_to, other, weights, m0)
    crossing1 = cross(m0, m1, pair_a, pair_b)
    (sums,) = call(
        keep_kernel,
        [shape((4 * PART, width), jnp.float32)],
        given,
        GRANT,
        scratch=scratch,
        **product,
    )(kept_for, own, weights, m0)
    kept0, m0, m1 = call(middle_kernel, [kept, small, small], [VMEM] * 3, 10)(sums, *crossing0)
    arrived0 = cross(m0, m1, pair_b, pair_a)
    kept1, m0, m1 = call(
        keep_middle_kernel,
        [kept, small, small],
        given + [VMEM] * 2,
        GRANT,
        scratch=[total] + scratch,
        **product,
    )(kept_for, other, weights, m0, *crossing1)
    arrived1 = cross(m0, m1, pair_b, pair_a)
    z = lax.axis_index("z").astype(jnp.int32)
    place = jnp.stack([core, z])
    piece = shape((TOK, width + 128), jnp.int16)
    grown = [pltpu.VMEM((2 * PART, width), jnp.float32)]
    final = []
    for q, (kept, arrived) in enumerate(((kept0, arrived0), (kept1, arrived1))):
        mine = shape((TOK, width), jnp.float32) if q == 0 else piece
        pieces = call(
            last_kernel, [mine] + [piece] * (NZ - 1), [SMEM] + [VMEM] * 3, 10, scratch=grown
        )(place, kept, *arrived)
        for k, sent in enumerate(pieces):
            if q == 0:
                final.append(sent if k == 0 else lax.ppermute(sent, "z", ring(NZ, k)))
            else:
                hops = [
                    (i * NC + c, (i + k) % NZ * NC + 1 - c)
                    for i in range(NZ)
                    for c in range(NC)
                ]
                final.append(lax.ppermute(sent, ("z", "c"), hops))
    return call(
        final_kernel, shape((1, TOK, full), jnp.bfloat16), [SMEM] + [VMEM] * (1 + 2 * NZ), 10
    )(place, bias, *final)


def solution(mesh):
    split = Mesh(mesh.devices.reshape(NZ, NY, NC, NX), ("z", "y", "c", "x"))
    lat = ("z", "y", "c")
    in_specs = (
        P((*lat, "x"), None, None),
        P((*lat, "x"), None),
        P((*lat, "x")),
        P(None, lat, "x"),
        P(None, "x"),
    )
    return jax.shard_map(
        run, mesh=split, in_specs=in_specs, out_specs=P(None, lat, "x"), check_vma=False
    )
```

```python
import jax
import jax.numpy as jnp
from jax import lax
from jax.experimental import pallas as pl
from jax.experimental.pallas import tpu as pltpu
from jax.sharding import Mesh
from jax.sharding import PartitionSpec as P


BLOCK = 128
MOST = 2
NZ, NY, NC, NX = 8, 4, 2, 4
CHIPS = NZ * NY
TOK = 32
OWN = 8
ACTIVE = 16
BLOCKS_DEV = 16
BLOCKS_CHIP = BLOCKS_DEV * NC
HALF = BLOCKS_DEV * MOST
SLOTS = BLOCKS_CHIP * MOST
ROWS = SLOTS + 8
PART = NZ // 2 * TOK
LIMIT = 32700.0
FLOOR = 2.0**-104
STEP = 256.0
LN2 = 0.6931471805599453
MIB = 1024 * 1024

VMEM = pl.BlockSpec(memory_space=pltpu.VMEM)
SMEM = pl.BlockSpec(memory_space=pltpu.SMEM)
HBM = pl.BlockSpec(memory_space=pltpu.HBM)
ANY = pl.BlockSpec(memory_space=pl.ANY)
PIECES = 4
GRANT = 18
WEIGHT_GRANT = 8


def ring(n, k):
    return [(i, (i + k) % n) for i in range(n)]


def call(kernel, out_shape, in_specs, mib, flops=0, scratch=()):
    return pl.pallas_call(
        kernel,
        out_shape=out_shape,
        in_specs=in_specs,
        out_specs=jax.tree.map(lambda _: VMEM, out_shape),
        scratch_shapes=list(scratch),
        compiler_params=pltpu.CompilerParams(vmem_limit_bytes=mib * MIB),
        cost_estimate=pl.CostEstimate(flops=flops, bytes_accessed=2 * MIB, transcendentals=0),
    )


def column(row):
    return jnp.transpose(jnp.broadcast_to(row, (128, 128)))


def wrap_kernel(counts_in, coeffs_in, ids_in, out_ref, counts, coeffs, ids, sems):
    n = OWN * ACTIVE
    copies = [
        pltpu.make_async_copy(ref, to, sems.at[k])
        for k, (ref, to) in enumerate(
            ((counts_in, counts), (coeffs_in, coeffs), (ids_in, ids))
        )
    ]
    for copy in copies:
        copy.start()
    for copy in copies:
        copy.wait()
    slot = lax.broadcasted_iota(jnp.int32, (ACTIVE, BLOCK), 0)
    for i in range(OWN):
        live = slot < counts[i]
        rows = jnp.where(live, coeffs[i].astype(jnp.float32), 0.0)
        out_ref[i * ACTIVE : (i + 1) * ACTIVE, :] = rows.astype(jnp.bfloat16)
    high = (ids[...] // 32).astype(jnp.float32)
    low = ids[...].astype(jnp.float32) - high * 32.0
    repeat = lax.broadcasted_iota(jnp.int32, (ACTIVE, n), 1) % ACTIVE
    repeat = jnp.where(repeat == lax.broadcasted_iota(jnp.int32, (ACTIVE, n), 0), 1.0, 0.0)
    token = lax.broadcasted_iota(jnp.int32, (OWN, n), 0)
    mine = lax.broadcasted_iota(jnp.int32, (OWN, n), 1) // ACTIVE == token
    meta = jnp.zeros((OWN, n), jnp.float32)
    for k, part in enumerate((high, low)):
        wide = jnp.dot(
            part.astype(jnp.bfloat16),
            repeat.astype(jnp.bfloat16),
            preferred_element_type=jnp.float32,
        )
        row = jnp.sum(jnp.where(mine, wide, 0.0), axis=0, keepdims=True)
        meta = jnp.where(token == k, jnp.broadcast_to(row, (OWN, n)), meta)
    out_ref[n : n + OWN, :] = meta.astype(jnp.bfloat16)


def pack_kernel(info, part0, part1, part2, part3, out_ref):
    parts = (part0, part1, part2, part3)
    n_part = OWN * ACTIVE
    ids = []
    for part in parts:
        meta = part[n_part : n_part + 8, :].astype(jnp.float32)
        ids.append(meta[0:1, :] * 32.0 + meta[1:2, :])
    ids_lane = jnp.concatenate(ids, axis=1)
    total = n_part * NX
    count = jnp.zeros((1, total), jnp.float32)
    lane = lax.broadcasted_iota(jnp.int32, (n_part, total), 1)
    sub = lax.broadcasted_iota(jnp.int32, (n_part, total), 0)
    for r in range(NX):
        col = column(ids[r])
        same = jnp.concatenate([col] * NX, axis=1) == ids_lane
        before = sub + r * n_part < lane
        count = count + jnp.sum(jnp.where(same & before, 1.0, 0.0), axis=0, keepdims=True)
    pos = ids_lane * float(MOST) + count
    dst = jnp.floor(pos * (1.0 / SLOTS))
    slot = pos - dst * SLOTS
    dst_row = lax.broadcasted_iota(jnp.int32, (CHIPS, n_part), 0).astype(jnp.float32)
    slot_lane = lax.broadcasted_iota(jnp.int32, (n_part, 128), 1).astype(jnp.float32)
    token = lax.broadcasted_iota(jnp.int32, (n_part, 128), 0) // ACTIVE
    meta = jnp.zeros((CHIPS, 128), jnp.float32)
    for r in range(NX):
        here = slice(r * n_part, (r + 1) * n_part)
        pick = jnp.where(dst[:, here] == dst_row, 1.0, 0.0).astype(jnp.bfloat16)
        first = lax.rem(info[0] - r + NX, NX) * OWN + 1
        named = (token + first).astype(jnp.float32)
        put = jnp.where(column(slot[:, here]) == slot_lane, named, 0.0).astype(jnp.bfloat16)
        meta = meta + jnp.dot(pick, put, preferred_element_type=jnp.float32)
    group = 4
    row = lax.broadcasted_iota(jnp.int32, (group * SLOTS, n_part), 0)
    for g in range(CHIPS // group):
        acc = jnp.zeros((group * SLOTS, BLOCK), jnp.float32)
        at = (row + g * group * SLOTS).astype(jnp.float32)
        for r in range(NX):
            here = slice(r * n_part, (r + 1) * n_part)
            hot = jnp.where(pos[:, here] == at, 1.0, 0.0).astype(jnp.bfloat16)
            acc = acc + jnp.dot(hot, parts[r][0:n_part, :], preferred_element_type=jnp.float32)
        acc = acc.astype(jnp.bfloat16)
        for k in range(group):
            d = g * group + k
            out_ref[d, 0:SLOTS, :] = acc[k * SLOTS : (k + 1) * SLOTS, :]
            out_ref[d, SLOTS:ROWS, :] = jnp.broadcast_to(meta[d : d + 1, :], (8, 128)).astype(
                jnp.bfloat16
            )


def prepare(info, arrived, tok_ref, coef_ref):
    core = info[0]
    meta = jnp.concatenate(
        [arrived[s, SLOTS:ROWS, :].astype(jnp.float32)[0:1, :] for s in range(CHIPS)]
        + [jnp.zeros((128 - CHIPS, 128), jnp.float32)],
        axis=0,
    )
    turned = jnp.transpose(meta)
    for s in range(CHIPS):
        for h in range(NC):
            to = pl.ds(pl.multiple_of(lax.rem(core + h, NC) * HALF, HALF), HALF)
            here = slice(h * HALF, (h + 1) * HALF)
            tok_ref[s, to, :] = jnp.broadcast_to(turned[here, s : s + 1], (HALF, 128))
            coef_ref[s, to, :] = arrived[s, here, :].astype(jnp.float32)


def quantized(acc):
    top = jnp.max(jnp.abs(acc), axis=1, keepdims=True)
    top = jnp.maximum(top, FLOOR) * (1.0 / LIMIT)
    code = jnp.ceil(jnp.log(top) * (STEP / LN2))
    scale = jnp.exp(code * (-LN2 / STEP))
    q = jnp.clip(jnp.floor(acc * scale + 0.5), -32767.0, 32767.0)
    return q.astype(jnp.int32).astype(jnp.int16), code


def write_message(out_ref, acc):
    n = acc.shape[0]
    q, code = quantized(acc)
    out_ref[0:n, :] = q
    for k in range(n // 128):
        lanes = jnp.transpose(jnp.broadcast_to(code[k * 128 : (k + 1) * 128, :], (128, 128)))
        out_ref[n : n + 8, k * 128 : (k + 1) * 128] = (
            lanes[0:8, :].astype(jnp.int32).astype(jnp.int16)
        )


def read_message(ref, k):
    n = ref.shape[0] - 8
    code = ref[n : n + 8, k * 128 : (k + 1) * 128]
    code = code.astype(jnp.int32).astype(jnp.float32)[0:1, :]
    scale = jnp.exp(column(code) * (LN2 / STEP))[:, 0:1]
    return ref[k * 128 : (k + 1) * 128, :].astype(jnp.int32).astype(jnp.float32) * scale


def weights_kernel(core_ref, w_own, w_other, after, out_ref, sems):
    depth, width = w_own.shape[1], out_ref.shape[1]
    columns = pl.ds(pl.multiple_of(core_ref[0] * width, 128), width)
    deep = NC * depth // PIECES
    copies = []
    for g in range(PIECES):
        ref = (w_own, w_other)[g // (PIECES // NC)]
        k = g % (PIECES // NC)
        copies.append(
            pltpu.make_async_copy(
                ref.at[0, k * deep : (k + 1) * deep, columns],
                out_ref.at[g * deep : (g + 1) * deep],
                sems.at[g],
            )
        )
    for copy in copies:
        copy.start()
    for copy in copies:
        copy.wait()


def build(rows_of, tok, coef, x_buf):
    t = lax.broadcasted_iota(jnp.int32, (TOK, 128), 0).astype(jnp.float32) + 1.0

    def source(i, carry):
        h, j, z = i // 8, (i // 4) % 2, i % 4
        first, second = jnp.where(h == 0, rows_of[0], rows_of[2]), jnp.where(
            h == 0, rows_of[1], rows_of[3]
        )
        n = (h * 4 + z) * NY + jnp.where(j == 0, first, second)
        base = pl.multiple_of(i * TOK, TOK)
        for b in range(BLOCKS_CHIP):
            row = jnp.zeros((TOK, 128), jnp.float32)
            for m in range(MOST):
                k = b * MOST + m
                hit = jnp.broadcast_to(tok[n, k : k + 1, :], (TOK, 128)) == t
                row = jnp.where(hit, jnp.broadcast_to(coef[n, k : k + 1, :], (TOK, 128)), row)
            x_buf[pl.ds(base, TOK), b * BLOCK : (b + 1) * BLOCK] = row.astype(jnp.bfloat16)
        return carry

    lax.fori_loop(0, 4 * PART // TOK, source, 0)


def multiply(send, core, y_ref, arrived, weights, tok, coef, x_buf, acc):
    y = y_ref[0]
    a, b = y + 1 - 2 * lax.rem(y, 2), NY - 1 - y
    opposite = NY - 1 - a
    prepare(core, arrived, tok, coef)
    build((a, opposite, b, opposite) if send else (y, b, y, a), tok, coef, x_buf)
    for h in range(2):
        here = slice(h * 2 * PART, (h + 1) * 2 * PART)
        acc[here, :] = jnp.dot(
            x_buf[here, :], weights[...], preferred_element_type=jnp.float32
        )


def send_kernel(core, y, arrived, weights, after, out0, out1, acc, *scratch):
    multiply(True, core, y, arrived, weights, *scratch, acc)
    for h, out in enumerate((out0, out1)):
        write_message(out, acc[h * 2 * PART : (h + 1) * 2 * PART, :])


def keep_kernel(core, y, arrived, weights, after, out_ref, *scratch):
    multiply(False, core, y, arrived, weights, *scratch, out_ref)


def keep_middle_kernel(
    core, y, arrived, weights, after, in0, in1, keep_ref, out0, out1, acc, *scratch
):
    multiply(False, core, y, arrived, weights, *scratch, acc)
    for h, (ref, out) in enumerate(((in0, out0), (in1, out1))):
        low, high = 2 * h * PART, (2 * h + 1) * PART
        keep_ref[h * PART : (h + 1) * PART, :] = acc[low:high, :] + read_message(ref, 0)
        write_message(out, acc[high : high + PART, :] + read_message(ref, 1))


def middle_kernel(kept, in0, in1, keep_ref, out0, out1):
    for h, (ref, out) in enumerate(((in0, out0), (in1, out1))):
        keep_ref[h * PART : (h + 1) * PART, :] = kept[
            2 * h * PART : (2 * h + 1) * PART, :
        ] + read_message(ref, 0)
        write_message(
            out, kept[(2 * h + 1) * PART : (2 * h + 2) * PART, :] + read_message(ref, 1)
        )


def last_kernel(info, *refs):
    ins, out_ref = refs[:-1], refs[-1]
    width = ins[0].shape[1]
    for q in range(NC):
        kept, messages = ins[3 * q], ins[3 * q + 1 : 3 * q + 3]
        c = lax.rem(info[0] + q, NC)
        for h, ref in enumerate(messages):
            acc = kept[h * PART : (h + 1) * PART, :] + read_message(ref, 0)
            v, code = quantized(acc)
            code = jnp.broadcast_to(code, (PART, 128)).astype(jnp.int32).astype(jnp.int16)
            for j in range(PART // TOK):
                d = (h * (PART // TOK) + j) * NC + c
                here = slice(j * TOK, (j + 1) * TOK)
                out_ref[d, :, 0:width] = v[here, :]
                out_ref[d, :, width : width + 128] = code[here, :]


def final_kernel(ref, bias, out_ref):
    width = out_ref.shape[2] // NC
    for c in range(NC):
        acc = jnp.broadcast_to(bias[:, c * width : (c + 1) * width], (TOK, width))
        for z in range(NZ):
            both = ref[z * NC + c].astype(jnp.int32).astype(jnp.float32)
            scale = jnp.exp(both[:, width : width + 1] * (LN2 / STEP))
            acc = acc + both[:, 0:width] * scale
        out_ref[0, :, c * width : (c + 1) * width] = acc.astype(jnp.bfloat16)


def run(coefficients, block_ids, counts, decoder, bias):
    core = lax.axis_index("c").astype(jnp.int32)
    x = lax.axis_index("x").astype(jnp.int32)
    y = lax.axis_index("y").astype(jnp.int32)
    depth, full = decoder.shape[1], decoder.shape[2]
    width = full // NC
    w_other = lax.ppermute(decoder, "c", ring(NC, 1))

    shape = jax.ShapeDtypeStruct
    packed = call(
        wrap_kernel,
        shape((OWN * (ACTIVE + 1), BLOCK), jnp.bfloat16),
        [HBM, HBM, HBM],
        10,
        scratch=[
            pltpu.SMEM((OWN,), jnp.int32),
            pltpu.VMEM((OWN, ACTIVE, BLOCK), jnp.bfloat16),
            pltpu.VMEM((OWN, ACTIVE), jnp.int32),
            pltpu.SemaphoreType.DMA((3,)),
        ],
    )(counts, coefficients, block_ids)
    parts = [packed] + [lax.ppermute(packed, "x", ring(NX, k)) for k in range(1, NX)]
    outgoing = call(
        pack_kernel, shape((CHIPS, ROWS, BLOCK), jnp.bfloat16), [SMEM] + [VMEM] * NX, 10
    )(x.reshape(1), *parts)
    own = lax.all_to_all(outgoing, ("z", "y"), 0, 0, tiled=True)
    weights = call(
        weights_kernel,
        shape((NC * depth, width), jnp.bfloat16),
        [SMEM, HBM, HBM, ANY],
        WEIGHT_GRANT,
        flops=10**10,
        scratch=[pltpu.SemaphoreType.DMA((PIECES,))],
    )(core.reshape(1), decoder, w_other, outgoing)
    other = lax.ppermute(own, "c", ring(NC, 1))
    pair_a, pair_b = [(i, i ^ 1) for i in range(NY)], [(i, NY - 1 - i) for i in range(NY)]
    place = (core.reshape(1), y.reshape(1))
    message = shape((2 * PART + 8, width), jnp.int16)
    small = shape((PART + 8, width), jnp.int16)

    kept = shape((2 * PART, width), jnp.float32)
    product = {"flops": 2 * 4 * PART * NC * depth * width}
    total = pltpu.VMEM((4 * PART, width), jnp.float32)
    scratch = [
        pltpu.VMEM((CHIPS, SLOTS, BLOCK), jnp.float32),
        pltpu.VMEM((CHIPS, SLOTS, BLOCK), jnp.float32),
        pltpu.VMEM((4 * PART, NC * depth), jnp.bfloat16),
    ]
    given = [SMEM, SMEM, VMEM, VMEM, ANY]

    def cross(m0, m1, pair0, pair1):
        m0 = lax.ppermute(m0, "y", pair0)
        m1 = lax.ppermute(m1, "y", pair1)
        return m0, m1

    m0, m1 = call(
        send_kernel, [message, message], given, GRANT, scratch=[total] + scratch, **product
    )(*place, own, weights, own)
    crossing0 = cross(m0, m1, pair_a, pair_b)
    m0, m1 = call(
        send_kernel, [message, message], given, GRANT, scratch=[total] + scratch, **product
    )(*place, other, weights, m0)
    crossing1 = cross(m0, m1, pair_a, pair_b)
    (sums,) = call(
        keep_kernel,
        [shape((4 * PART, width), jnp.float32)],
        given,
        GRANT,
        scratch=scratch,
        **product,
    )(*place, own, weights, m0)
    kept0, m0, m1 = call(middle_kernel, [kept, small, small], [VMEM] * 3, 10)(sums, *crossing0)
    arrived0 = cross(m0, m1, pair_b, pair_a)
    kept1, m0, m1 = call(
        keep_middle_kernel,
        [kept, small, small],
        given + [VMEM] * 2,
        GRANT,
        scratch=[total] + scratch,
        **product,
    )(*place, other, weights, m0, *crossing1)
    arrived1 = cross(m0, m1, pair_b, pair_a)
    out = call(
        last_kernel, shape((NZ * NC, TOK, width + 128), jnp.int16), [SMEM] + [VMEM] * 6, 10
    )(core.reshape(1), kept0, *arrived0, kept1, *arrived1)
    return call(
        final_kernel, shape((1, TOK, full), jnp.bfloat16), [VMEM] * 2, 10
    )(lax.all_to_all(out, ("z", "c"), 0, 0, tiled=True), bias)


def solution(mesh):
    split = Mesh(mesh.devices.reshape(NZ, NY, NC, NX), ("z", "y", "c", "x"))
    lat = ("z", "y", "c")
    in_specs = (
        P((*lat, "x"), None, None),
        P((*lat, "x"), None),
        P((*lat, "x")),
        P(None, lat, "x"),
        P(None, "x"),
    )
    return jax.shard_map(
        run, mesh=split, in_specs=in_specs, out_specs=P(None, lat, "x"), check_vma=False
    )
```

```python
import jax
import jax.numpy as jnp
from jax import lax
from jax.experimental import pallas as pl
from jax.experimental.pallas import tpu as pltpu
from jax.sharding import Mesh
from jax.sharding import PartitionSpec as P


BLOCK = 128
MOST = 2
NZ, NY, NC, NX = 8, 4, 2, 4
CHIPS = NZ * NY
TOK = 32
OWN = 8
ACTIVE = 16
BLOCKS_DEV = 16
BLOCKS_CHIP = BLOCKS_DEV * NC
HALF = BLOCKS_DEV * MOST
SLOTS = BLOCKS_CHIP * MOST
ROWS = SLOTS + 8
PART = NZ // 2 * TOK
LIMIT = 32700.0
FLOOR = 2.0**-104
STEP = 256.0
LN2 = 0.6931471805599453
MIB = 1024 * 1024

VMEM = pl.BlockSpec(memory_space=pltpu.VMEM)
SMEM = pl.BlockSpec(memory_space=pltpu.SMEM)
HBM = pl.BlockSpec(memory_space=pltpu.HBM)
ANY = pl.BlockSpec(memory_space=pl.ANY)
PIECES = 4
GRANT = 18
FIRST_GRANT = 44
FIRST = 1024
WEIGHT_GRANT = 50


def ring(n, k):
    return [(i, (i + k) % n) for i in range(n)]


def call(kernel, out_shape, in_specs, mib, flops=0, scratch=()):
    return pl.pallas_call(
        kernel,
        out_shape=out_shape,
        in_specs=in_specs,
        out_specs=jax.tree.map(lambda _: VMEM, out_shape),
        scratch_shapes=list(scratch),
        compiler_params=pltpu.CompilerParams(vmem_limit_bytes=mib * MIB),
        cost_estimate=pl.CostEstimate(flops=flops, bytes_accessed=2 * MIB, transcendentals=0),
    )


def column(row):
    return jnp.transpose(jnp.broadcast_to(row, (128, 128)))


def wrap_kernel(counts_in, coeffs_in, ids_in, out_ref, counts, coeffs, ids, sems):
    n = OWN * ACTIVE
    copies = [
        pltpu.make_async_copy(ref, to, sems.at[k])
        for k, (ref, to) in enumerate(
            ((counts_in, counts), (coeffs_in, coeffs), (ids_in, ids))
        )
    ]
    for copy in copies:
        copy.start()
    for copy in copies:
        copy.wait()
    slot = lax.broadcasted_iota(jnp.int32, (ACTIVE, BLOCK), 0)
    for i in range(OWN):
        live = slot < counts[i]
        rows = jnp.where(live, coeffs[i].astype(jnp.float32), 0.0)
        out_ref[i * ACTIVE : (i + 1) * ACTIVE, :] = rows.astype(jnp.bfloat16)
    high = (ids[...] // 32).astype(jnp.float32)
    low = ids[...].astype(jnp.float32) - high * 32.0
    repeat = lax.broadcasted_iota(jnp.int32, (ACTIVE, n), 1) % ACTIVE
    repeat = jnp.where(repeat == lax.broadcasted_iota(jnp.int32, (ACTIVE, n), 0), 1.0, 0.0)
    token = lax.broadcasted_iota(jnp.int32, (OWN, n), 0)
    mine = lax.broadcasted_iota(jnp.int32, (OWN, n), 1) // ACTIVE == token
    meta = jnp.zeros((OWN, n), jnp.float32)
    for k, part in enumerate((high, low)):
        wide = jnp.dot(
            part.astype(jnp.bfloat16),
            repeat.astype(jnp.bfloat16),
            preferred_element_type=jnp.float32,
        )
        row = jnp.sum(jnp.where(mine, wide, 0.0), axis=0, keepdims=True)
        meta = jnp.where(token == k, jnp.broadcast_to(row, (OWN, n)), meta)
    out_ref[n : n + OWN, :] = meta.astype(jnp.bfloat16)


def pack_kernel(info, part0, part1, part2, part3, out_ref, buf, sems):
    parts = (part0, part1, part2, part3)
    n_part = OWN * ACTIVE
    ids = []
    for part in parts:
        meta = part[n_part : n_part + 8, :].astype(jnp.float32)
        ids.append(meta[0:1, :] * 32.0 + meta[1:2, :])
    ids_lane = jnp.concatenate(ids, axis=1)
    total = n_part * NX
    count = jnp.zeros((1, total), jnp.float32)
    lane = lax.broadcasted_iota(jnp.int32, (n_part, total), 1)
    sub = lax.broadcasted_iota(jnp.int32, (n_part, total), 0)
    for r in range(NX):
        col = column(ids[r])
        same = jnp.concatenate([col] * NX, axis=1) == ids_lane
        before = sub + r * n_part < lane
        count = count + jnp.sum(jnp.where(same & before, 1.0, 0.0), axis=0, keepdims=True)
    pos = ids_lane * float(MOST) + count
    dst = jnp.floor(pos * (1.0 / SLOTS))
    slot = pos - dst * SLOTS
    dst_row = lax.broadcasted_iota(jnp.int32, (CHIPS, n_part), 0).astype(jnp.float32)
    slot_lane = lax.broadcasted_iota(jnp.int32, (n_part, 128), 1).astype(jnp.float32)
    token = lax.broadcasted_iota(jnp.int32, (n_part, 128), 0) // ACTIVE
    meta = jnp.zeros((CHIPS, 128), jnp.float32)
    for r in range(NX):
        here = slice(r * n_part, (r + 1) * n_part)
        pick = jnp.where(dst[:, here] == dst_row, 1.0, 0.0).astype(jnp.bfloat16)
        first = lax.rem(info[0] - r + NX, NX) * OWN + 1
        named = (token + first).astype(jnp.float32)
        put = jnp.where(column(slot[:, here]) == slot_lane, named, 0.0).astype(jnp.bfloat16)
        meta = meta + jnp.dot(pick, put, preferred_element_type=jnp.float32)
    group = 4
    copies = []
    for g in range(CHIPS // group):
        here = slice(g * group, (g + 1) * group)
        copies.append(pltpu.make_async_copy(buf.at[here], out_ref.at[here], sems.at[g]))
    row = lax.broadcasted_iota(jnp.int32, (group * SLOTS, n_part), 0)
    for g in range(CHIPS // group):
        acc = jnp.zeros((group * SLOTS, BLOCK), jnp.float32)
        at = (row + g * group * SLOTS).astype(jnp.float32)
        for r in range(NX):
            here = slice(r * n_part, (r + 1) * n_part)
            hot = jnp.where(pos[:, here] == at, 1.0, 0.0).astype(jnp.bfloat16)
            acc = acc + jnp.dot(hot, parts[r][0:n_part, :], preferred_element_type=jnp.float32)
        acc = acc.astype(jnp.bfloat16)
        for k in range(group):
            d = g * group + k
            buf[d, 0:SLOTS, :] = acc[k * SLOTS : (k + 1) * SLOTS, :]
            buf[d, SLOTS:ROWS, :] = jnp.broadcast_to(meta[d : d + 1, :], (8, 128)).astype(
                jnp.bfloat16
            )
        if g > 0:
            copies[g - 1].start()
    copies[-1].start()
    for copy in copies:
        copy.wait()


def prepare(info, arrived, tok_ref, coef_ref):
    core = info[0]
    meta = jnp.concatenate(
        [arrived[s, SLOTS:ROWS, :].astype(jnp.float32)[0:1, :] for s in range(CHIPS)]
        + [jnp.zeros((128 - CHIPS, 128), jnp.float32)],
        axis=0,
    )
    turned = jnp.transpose(meta)
    for s in range(CHIPS):
        for h in range(NC):
            to = pl.ds(pl.multiple_of(lax.rem(core + h, NC) * HALF, HALF), HALF)
            here = slice(h * HALF, (h + 1) * HALF)
            tok_ref[s, to, :] = jnp.broadcast_to(turned[here, s : s + 1], (HALF, 128))
            coef_ref[s, to, :] = arrived[s, here, :].astype(jnp.float32)


def quantized(acc):
    top = jnp.max(jnp.abs(acc), axis=1, keepdims=True)
    top = jnp.maximum(top, FLOOR) * (1.0 / LIMIT)
    code = jnp.ceil(jnp.log(top) * (STEP / LN2))
    scale = jnp.exp(code * (-LN2 / STEP))
    q = jnp.clip(jnp.floor(acc * scale + 0.5), -32767.0, 32767.0)
    return q.astype(jnp.int32).astype(jnp.int16), code


def write_message(out_ref, acc):
    n = acc.shape[0]
    q, code = quantized(acc)
    out_ref[0:n, :] = q
    for k in range(n // 128):
        lanes = jnp.transpose(jnp.broadcast_to(code[k * 128 : (k + 1) * 128, :], (128, 128)))
        out_ref[n : n + 8, k * 128 : (k + 1) * 128] = (
            lanes[0:8, :].astype(jnp.int32).astype(jnp.int16)
        )


def read_message(ref, k):
    n = ref.shape[0] - 8
    code = ref[n : n + 8, k * 128 : (k + 1) * 128]
    code = code.astype(jnp.int32).astype(jnp.float32)[0:1, :]
    scale = jnp.exp(column(code) * (LN2 / STEP))[:, 0:1]
    return ref[k * 128 : (k + 1) * 128, :].astype(jnp.int32).astype(jnp.float32) * scale


def weights_kernel(core_ref, w_own, w_other, after, out_ref, sems):
    depth, width = w_own.shape[1], out_ref.shape[1]
    columns = pl.ds(pl.multiple_of(core_ref[0] * width, 128), width)
    deep = NC * depth // PIECES
    copies = []
    for g in range(PIECES):
        ref = (w_own, w_other)[g // (PIECES // NC)]
        k = g % (PIECES // NC)
        copies.append(
            pltpu.make_async_copy(
                ref.at[0, k * deep : (k + 1) * deep, columns],
                out_ref.at[g * deep : (g + 1) * deep],
                sems.at[g],
            )
        )
    for copy in copies:
        copy.start()
    for copy in copies:
        copy.wait()


def build(rows_of, tok, coef, x_buf):
    t = lax.broadcasted_iota(jnp.int32, (TOK, 128), 0).astype(jnp.float32) + 1.0

    def source(i, carry):
        h, j, z = i // 8, (i // 4) % 2, i % 4
        first, second = jnp.where(h == 0, rows_of[0], rows_of[2]), jnp.where(
            h == 0, rows_of[1], rows_of[3]
        )
        n = (h * 4 + z) * NY + jnp.where(j == 0, first, second)
        base = pl.multiple_of(i * TOK, TOK)
        for b in range(BLOCKS_CHIP):
            row = jnp.zeros((TOK, 128), jnp.float32)
            for m in range(MOST):
                k = b * MOST + m
                hit = jnp.broadcast_to(tok[n, k : k + 1, :], (TOK, 128)) == t
                row = jnp.where(hit, jnp.broadcast_to(coef[n, k : k + 1, :], (TOK, 128)), row)
            x_buf[pl.ds(base, TOK), b * BLOCK : (b + 1) * BLOCK] = row.astype(jnp.bfloat16)
        return carry

    lax.fori_loop(0, 4 * PART // TOK, source, 0)


def multiply(send, core, y_ref, arrived, weights, tok, coef, x_buf, acc):
    y = y_ref[0]
    a, b = y + 1 - 2 * lax.rem(y, 2), NY - 1 - y
    opposite = NY - 1 - a
    prepare(core, arrived, tok, coef)
    build((a, opposite, b, opposite) if send else (y, b, y, a), tok, coef, x_buf)
    for h in range(2):
        here = slice(h * 2 * PART, (h + 1) * 2 * PART)
        acc[here, :] = jnp.dot(
            x_buf[here, :], weights[...], preferred_element_type=jnp.float32
        )


def first_kernel(core, y, arrived, weights, out0, out1, w_ref, acc, tok, coef, x_buf, sems):
    pieces = (slice(0, FIRST), slice(FIRST, w_ref.shape[0]))
    copies = [
        pltpu.make_async_copy(weights.at[here], w_ref.at[here], sems.at[g])
        for g, here in enumerate(pieces)
    ]
    copies[0].start()
    a, b = y[0] + 1 - 2 * lax.rem(y[0], 2), NY - 1 - y[0]
    opposite = NY - 1 - a
    prepare(core, arrived, tok, coef)
    copies[1].start()
    build((a, opposite, b, opposite), tok, coef, x_buf)
    for g, (copy, here) in enumerate(zip(copies, pieces, strict=True)):
        copy.wait()
        for h in range(2):
            rows = slice(h * 2 * PART, (h + 1) * 2 * PART)
            term = jnp.dot(
                x_buf[rows, here], w_ref[here, :], preferred_element_type=jnp.float32
            )
            if g == 0:
                acc[rows, :] = term
            else:
                write_message((out0, out1)[h], acc[rows, :] + term)


def send_kernel(core, y, arrived, weights, after, out0, out1, acc, *scratch):
    multiply(True, core, y, arrived, weights, *scratch, acc)
    for h, out in enumerate((out0, out1)):
        write_message(out, acc[h * 2 * PART : (h + 1) * 2 * PART, :])


def keep_kernel(core, y, arrived, weights, after, out_ref, *scratch):
    multiply(False, core, y, arrived, weights, *scratch, out_ref)


def keep_middle_kernel(
    core, y, arrived, weights, after, in0, in1, keep_ref, out0, out1, acc, *scratch
):
    multiply(False, core, y, arrived, weights, *scratch, acc)
    for h, (ref, out) in enumerate(((in0, out0), (in1, out1))):
        low, high = 2 * h * PART, (2 * h + 1) * PART
        keep_ref[h * PART : (h + 1) * PART, :] = acc[low:high, :] + read_message(ref, 0)
        write_message(out, acc[high : high + PART, :] + read_message(ref, 1))


def middle_kernel(kept, in0, in1, keep_ref, out0, out1):
    for h, (ref, out) in enumerate(((in0, out0), (in1, out1))):
        keep_ref[h * PART : (h + 1) * PART, :] = kept[
            2 * h * PART : (2 * h + 1) * PART, :
        ] + read_message(ref, 0)
        write_message(
            out, kept[(2 * h + 1) * PART : (2 * h + 2) * PART, :] + read_message(ref, 1)
        )


def last_kernel(info, *refs):
    ins, out_ref = refs[:-1], refs[-1]
    width = ins[0].shape[1]
    for q in range(NC):
        kept, messages = ins[3 * q], ins[3 * q + 1 : 3 * q + 3]
        c = lax.rem(info[0] + q, NC)
        for h, ref in enumerate(messages):
            acc = kept[h * PART : (h + 1) * PART, :] + read_message(ref, 0)
            v, code = quantized(acc)
            code = jnp.broadcast_to(code, (PART, 128)).astype(jnp.int32).astype(jnp.int16)
            for j in range(PART // TOK):
                d = (h * (PART // TOK) + j) * NC + c
                here = slice(j * TOK, (j + 1) * TOK)
                out_ref[d, :, 0:width] = v[here, :]
                out_ref[d, :, width : width + 128] = code[here, :]


def final_kernel(ref, bias, out_ref):
    width = out_ref.shape[2] // NC
    for c in range(NC):
        acc = jnp.broadcast_to(bias[:, c * width : (c + 1) * width], (TOK, width))
        for z in range(NZ):
            both = ref[z * NC + c].astype(jnp.int32).astype(jnp.float32)
            scale = jnp.exp(both[:, width : width + 1] * (LN2 / STEP))
            acc = acc + both[:, 0:width] * scale
        out_ref[0, :, c * width : (c + 1) * width] = acc.astype(jnp.bfloat16)


def run(coefficients, block_ids, counts, decoder, bias):
    core = lax.axis_index("c").astype(jnp.int32)
    x = lax.axis_index("x").astype(jnp.int32)
    y = lax.axis_index("y").astype(jnp.int32)
    depth, full = decoder.shape[1], decoder.shape[2]
    width = full // NC
    w_other = lax.ppermute(decoder, "c", ring(NC, 1))

    shape = jax.ShapeDtypeStruct
    packed = call(
        wrap_kernel,
        shape((OWN * (ACTIVE + 1), BLOCK), jnp.bfloat16),
        [HBM, HBM, HBM],
        10,
        scratch=[
            pltpu.SMEM((OWN,), jnp.int32),
            pltpu.VMEM((OWN, ACTIVE, BLOCK), jnp.bfloat16),
            pltpu.VMEM((OWN, ACTIVE), jnp.int32),
            pltpu.SemaphoreType.DMA((3,)),
        ],
    )(counts, coefficients, block_ids)
    parts = [packed] + [lax.ppermute(packed, "x", ring(NX, k)) for k in range(1, NX)]
    outgoing = pl.pallas_call(
        pack_kernel,
        out_shape=shape((CHIPS, ROWS, BLOCK), jnp.bfloat16),
        in_specs=[SMEM] + [VMEM] * NX,
        out_specs=HBM,
        scratch_shapes=[
            pltpu.VMEM((CHIPS, ROWS, BLOCK), jnp.bfloat16),
            pltpu.SemaphoreType.DMA((CHIPS // 4,)),
        ],
        compiler_params=pltpu.CompilerParams(vmem_limit_bytes=10 * MIB),
        name="pack",
    )(x.reshape(1), *parts)
    own = lax.all_to_all(outgoing, ("z", "y"), 0, 0, tiled=True)
    weights = call(
        weights_kernel,
        shape((NC * depth, width), jnp.bfloat16),
        [SMEM, HBM, HBM, ANY],
        WEIGHT_GRANT,
        flops=10**10,
        scratch=[pltpu.SemaphoreType.DMA((PIECES,))],
    )(core.reshape(1), decoder, w_other, outgoing)
    other = lax.ppermute(own, "c", ring(NC, 1))
    pair_a, pair_b = [(i, i ^ 1) for i in range(NY)], [(i, NY - 1 - i) for i in range(NY)]
    place = (core.reshape(1), y.reshape(1))
    message = shape((2 * PART + 8, width), jnp.int16)
    small = shape((PART + 8, width), jnp.int16)

    kept = shape((2 * PART, width), jnp.float32)
    product = {"flops": 2 * 4 * PART * NC * depth * width}
    total = pltpu.VMEM((4 * PART, width), jnp.float32)
    scratch = [
        pltpu.VMEM((CHIPS, SLOTS, BLOCK), jnp.float32),
        pltpu.VMEM((CHIPS, SLOTS, BLOCK), jnp.float32),
        pltpu.VMEM((4 * PART, NC * depth), jnp.bfloat16),
    ]
    given = [SMEM, SMEM, VMEM, VMEM, ANY]

    def cross(m0, m1, pair0, pair1):
        m0 = lax.ppermute(m0, "y", pair0)
        m1 = lax.ppermute(m1, "y", pair1)
        return m0, m1

    m0, m1, weights = call(
        first_kernel,
        [message, message, shape((NC * depth, width), jnp.bfloat16)],
        [SMEM, SMEM, VMEM, HBM],
        FIRST_GRANT,
        scratch=[total, *scratch, pltpu.SemaphoreType.DMA((2,))],
        **product,
    )(*place, own, weights)
    crossing0 = cross(m0, m1, pair_a, pair_b)
    m0, m1 = call(
        send_kernel, [message, message], given, GRANT, scratch=[total] + scratch, **product
    )(*place, other, weights, m0)
    crossing1 = cross(m0, m1, pair_a, pair_b)
    (sums,) = call(
        keep_kernel,
        [shape((4 * PART, width), jnp.float32)],
        given,
        GRANT,
        scratch=scratch,
        **product,
    )(*place, own, weights, m0)
    kept0, m0, m1 = call(middle_kernel, [kept, small, small], [VMEM] * 3, 10)(sums, *crossing0)
    arrived0 = cross(m0, m1, pair_b, pair_a)
    kept1, m0, m1 = call(
        keep_middle_kernel,
        [kept, small, small],
        given + [VMEM] * 2,
        GRANT,
        scratch=[total] + scratch,
        **product,
    )(*place, other, weights, m0, *crossing1)
    arrived1 = cross(m0, m1, pair_b, pair_a)
    out = call(
        last_kernel, shape((NZ * NC, TOK, width + 128), jnp.int16), [SMEM] + [VMEM] * 6, 10
    )(core.reshape(1), kept0, *arrived0, kept1, *arrived1)
    return call(
        final_kernel, shape((1, TOK, full), jnp.bfloat16), [VMEM] * 2, 10
    )(lax.all_to_all(out, ("z", "c"), 0, 0, tiled=True), bias)


def solution(mesh):
    split = Mesh(mesh.devices.reshape(NZ, NY, NC, NX), ("z", "y", "c", "x"))
    lat = ("z", "y", "c")
    in_specs = (
        P((*lat, "x"), None, None),
        P((*lat, "x"), None),
        P((*lat, "x")),
        P(None, lat, "x"),
        P(None, "x"),
    )
    return jax.shard_map(
        run, mesh=split, in_specs=in_specs, out_specs=P(None, lat, "x"), check_vma=False
    )
```

```python
import functools

import jax
import jax.numpy as jnp
from jax import lax
from jax.experimental import pallas as pl
from jax.experimental.pallas import tpu as pltpu
from jax.sharding import Mesh
from jax.sharding import PartitionSpec as P


BLOCK = 128
MOST = 2
NZ, NY, NC, NX = 8, 4, 2, 4
CHIPS = NZ * NY
TOK = 32
OWN = 8
ACTIVE = 16
BLOCKS_DEV = 16
BLOCKS_CHIP = BLOCKS_DEV * NC
HALF = BLOCKS_DEV * MOST
SLOTS = BLOCKS_CHIP * MOST
ROWS = SLOTS + 8
PART = NZ // 2 * TOK
LIMIT = 32700.0
FLOOR = 2.0**-104
STEP = 256.0
LN2 = 0.6931471805599453
MIB = 1024 * 1024

VMEM = pl.BlockSpec(memory_space=pltpu.VMEM)
SMEM = pl.BlockSpec(memory_space=pltpu.SMEM)
HBM = pl.BlockSpec(memory_space=pltpu.HBM)
ANY = pl.BlockSpec(memory_space=pl.ANY)
PIECES = 4
GRANT = 18
FIRST_GRANT = 44
FIRST = 1024
WEIGHT_GRANT = 50


def ring(n, k):
    return [(i, (i + k) % n) for i in range(n)]


def call(kernel, out_shape, in_specs, mib, flops=0, scratch=()):
    return pl.pallas_call(
        kernel,
        out_shape=out_shape,
        in_specs=in_specs,
        out_specs=jax.tree.map(lambda _: VMEM, out_shape),
        scratch_shapes=list(scratch),
        compiler_params=pltpu.CompilerParams(vmem_limit_bytes=mib * MIB),
        cost_estimate=pl.CostEstimate(flops=flops, bytes_accessed=2 * MIB, transcendentals=0),
    )


def column(row):
    return jnp.transpose(jnp.broadcast_to(row, (128, 128)))


def wrap_kernel(counts_in, coeffs_in, ids_in, out_ref, counts, coeffs, ids, sems):
    n = OWN * ACTIVE
    copies = [
        pltpu.make_async_copy(ref, to, sems.at[k])
        for k, (ref, to) in enumerate(
            ((counts_in, counts), (coeffs_in, coeffs), (ids_in, ids))
        )
    ]
    for copy in copies:
        copy.start()
    for copy in copies:
        copy.wait()
    slot = lax.broadcasted_iota(jnp.int32, (ACTIVE, BLOCK), 0)
    for i in range(OWN):
        live = slot < counts[i]
        rows = jnp.where(live, coeffs[i].astype(jnp.float32), 0.0)
        out_ref[i * ACTIVE : (i + 1) * ACTIVE, :] = rows.astype(jnp.bfloat16)
    high = (ids[...] // 32).astype(jnp.float32)
    low = ids[...].astype(jnp.float32) - high * 32.0
    repeat = lax.broadcasted_iota(jnp.int32, (ACTIVE, n), 1) % ACTIVE
    repeat = jnp.where(repeat == lax.broadcasted_iota(jnp.int32, (ACTIVE, n), 0), 1.0, 0.0)
    token = lax.broadcasted_iota(jnp.int32, (OWN, n), 0)
    mine = lax.broadcasted_iota(jnp.int32, (OWN, n), 1) // ACTIVE == token
    meta = jnp.zeros((OWN, n), jnp.float32)
    for k, part in enumerate((high, low)):
        wide = jnp.dot(
            part.astype(jnp.bfloat16),
            repeat.astype(jnp.bfloat16),
            preferred_element_type=jnp.float32,
        )
        row = jnp.sum(jnp.where(mine, wide, 0.0), axis=0, keepdims=True)
        meta = jnp.where(token == k, jnp.broadcast_to(row, (OWN, n)), meta)
    out_ref[n : n + OWN, :] = meta.astype(jnp.bfloat16)


def pack_kernel(info, part0, part1, part2, part3, out_ref, buf, sems):
    parts = (part0, part1, part2, part3)
    n_part = OWN * ACTIVE
    ids = []
    for part in parts:
        meta = part[n_part : n_part + 8, :].astype(jnp.float32)
        ids.append(meta[0:1, :] * 32.0 + meta[1:2, :])
    ids_lane = jnp.concatenate(ids, axis=1)
    total = n_part * NX
    count = jnp.zeros((1, total), jnp.float32)
    lane = lax.broadcasted_iota(jnp.int32, (n_part, total), 1)
    sub = lax.broadcasted_iota(jnp.int32, (n_part, total), 0)
    for r in range(NX):
        col = column(ids[r])
        same = jnp.concatenate([col] * NX, axis=1) == ids_lane
        before = sub + r * n_part < lane
        count = count + jnp.sum(jnp.where(same & before, 1.0, 0.0), axis=0, keepdims=True)
    pos = ids_lane * float(MOST) + count
    dst = jnp.floor(pos * (1.0 / SLOTS))
    slot = pos - dst * SLOTS
    dst_row = lax.broadcasted_iota(jnp.int32, (CHIPS, n_part), 0).astype(jnp.float32)
    slot_lane = lax.broadcasted_iota(jnp.int32, (n_part, 128), 1).astype(jnp.float32)
    token = lax.broadcasted_iota(jnp.int32, (n_part, 128), 0) // ACTIVE
    meta = jnp.zeros((CHIPS, 128), jnp.float32)
    for r in range(NX):
        here = slice(r * n_part, (r + 1) * n_part)
        pick = jnp.where(dst[:, here] == dst_row, 1.0, 0.0).astype(jnp.bfloat16)
        first = lax.rem(info[0] - r + NX, NX) * OWN + 1
        named = (token + first).astype(jnp.float32)
        put = jnp.where(column(slot[:, here]) == slot_lane, named, 0.0).astype(jnp.bfloat16)
        meta = meta + jnp.dot(pick, put, preferred_element_type=jnp.float32)
    group = 4
    copies = []
    for g in range(CHIPS // group):
        here = slice(g * group, (g + 1) * group)
        copies.append(pltpu.make_async_copy(buf.at[here], out_ref.at[here], sems.at[g]))
    row = lax.broadcasted_iota(jnp.int32, (group * SLOTS, n_part), 0)
    for g in range(CHIPS // group):
        acc = jnp.zeros((group * SLOTS, BLOCK), jnp.float32)
        at = (row + g * group * SLOTS).astype(jnp.float32)
        for r in range(NX):
            here = slice(r * n_part, (r + 1) * n_part)
            hot = jnp.where(pos[:, here] == at, 1.0, 0.0).astype(jnp.bfloat16)
            acc = acc + jnp.dot(hot, parts[r][0:n_part, :], preferred_element_type=jnp.float32)
        acc = acc.astype(jnp.bfloat16)
        for k in range(group):
            d = g * group + k
            buf[d, 0:SLOTS, :] = acc[k * SLOTS : (k + 1) * SLOTS, :]
            buf[d, SLOTS:ROWS, :] = jnp.broadcast_to(meta[d : d + 1, :], (8, 128)).astype(
                jnp.bfloat16
            )
        if g > 0:
            copies[g - 1].start()
    copies[-1].start()
    for copy in copies:
        copy.wait()


def prepare(info, arrived, tok_ref, coef_ref):
    core = info[0]
    meta = jnp.concatenate(
        [arrived[s, SLOTS:ROWS, :].astype(jnp.float32)[0:1, :] for s in range(CHIPS)]
        + [jnp.zeros((128 - CHIPS, 128), jnp.float32)],
        axis=0,
    )
    turned = jnp.transpose(meta)
    for s in range(CHIPS):
        for h in range(NC):
            to = pl.ds(pl.multiple_of(lax.rem(core + h, NC) * HALF, HALF), HALF)
            here = slice(h * HALF, (h + 1) * HALF)
            tok_ref[s, to, :] = jnp.broadcast_to(turned[here, s : s + 1], (HALF, 128))
            coef_ref[s, to, :] = arrived[s, here, :].astype(jnp.float32)


def quantized(acc):
    top = jnp.max(jnp.abs(acc), axis=1, keepdims=True)
    top = jnp.maximum(top, FLOOR) * (1.0 / LIMIT)
    code = jnp.ceil(jnp.log(top) * (STEP / LN2))
    scale = jnp.exp(code * (-LN2 / STEP))
    q = jnp.clip(jnp.floor(acc * scale + 0.5), -32767.0, 32767.0)
    return q.astype(jnp.int32).astype(jnp.int16), code


def write_message(out_ref, acc):
    n = acc.shape[0]
    q, code = quantized(acc)
    out_ref[0:n, :] = q
    for k in range(n // 128):
        lanes = jnp.transpose(jnp.broadcast_to(code[k * 128 : (k + 1) * 128, :], (128, 128)))
        out_ref[n : n + 8, k * 128 : (k + 1) * 128] = (
            lanes[0:8, :].astype(jnp.int32).astype(jnp.int16)
        )


def read_message(ref, k):
    n = ref.shape[0] - 8
    code = ref[n : n + 8, k * 128 : (k + 1) * 128]
    code = code.astype(jnp.int32).astype(jnp.float32)[0:1, :]
    scale = jnp.exp(column(code) * (LN2 / STEP))[:, 0:1]
    return ref[k * 128 : (k + 1) * 128, :].astype(jnp.int32).astype(jnp.float32) * scale


def weights_kernel(core_ref, w_own, w_other, after, out_ref, sems):
    depth, width = w_own.shape[1], out_ref.shape[1]
    columns = pl.ds(pl.multiple_of(core_ref[0] * width, 128), width)
    deep = NC * depth // PIECES
    copies = []
    for g in range(PIECES):
        ref = (w_own, w_other)[g // (PIECES // NC)]
        k = g % (PIECES // NC)
        copies.append(
            pltpu.make_async_copy(
                ref.at[0, k * deep : (k + 1) * deep, columns],
                out_ref.at[g * deep : (g + 1) * deep],
                sems.at[g],
            )
        )
    for copy in copies:
        copy.start()
    for copy in copies:
        copy.wait()


def build(rows_of, tok, coef, x_buf):
    t = lax.broadcasted_iota(jnp.int32, (TOK, 128), 0).astype(jnp.float32) + 1.0

    def source(i, carry):
        each = len(rows_of) // 2
        h, j, z = i // (4 * each), (i // 4) % each, i % 4
        y = rows_of[-1]
        for k in range(len(rows_of) - 1):
            y = jnp.where(h * each + j == k, rows_of[k], y)
        n = (h * 4 + z) * NY + y
        base = pl.multiple_of(i * TOK, TOK)
        for b in range(BLOCKS_CHIP):
            row = jnp.zeros((TOK, 128), jnp.float32)
            for m in range(MOST):
                k = b * MOST + m
                hit = jnp.broadcast_to(tok[n, k : k + 1, :], (TOK, 128)) == t
                row = jnp.where(hit, jnp.broadcast_to(coef[n, k : k + 1, :], (TOK, 128)), row)
            x_buf[pl.ds(base, TOK), b * BLOCK : (b + 1) * BLOCK] = row.astype(jnp.bfloat16)
        return carry

    lax.fori_loop(0, len(rows_of) * PART // TOK, source, 0)


def multiply(send, core, y_ref, arrived, weights, tok, coef, x_buf, acc):
    y = y_ref[0]
    a, b = y + 1 - 2 * lax.rem(y, 2), NY - 1 - y
    opposite = NY - 1 - a
    prepare(core, arrived, tok, coef)
    build((a, opposite, b, opposite) if send else (y, b, y, a), tok, coef, x_buf)
    for h in range(2):
        here = slice(h * 2 * PART, (h + 1) * 2 * PART)
        acc[here, :] = jnp.dot(
            x_buf[here, :], weights[...], preferred_element_type=jnp.float32
        )


def first_kernel(core, y, arrived, weights, out0, out1, w_ref, acc, tok, coef, x_buf, sems):
    pieces = (slice(0, FIRST), slice(FIRST, w_ref.shape[0]))
    copies = [
        pltpu.make_async_copy(weights.at[here], w_ref.at[here], sems.at[g])
        for g, here in enumerate(pieces)
    ]
    copies[0].start()
    a, b = y[0] + 1 - 2 * lax.rem(y[0], 2), NY - 1 - y[0]
    opposite = NY - 1 - a
    prepare(core, arrived, tok, coef)
    copies[1].start()
    build((a, opposite, b, opposite), tok, coef, x_buf)
    for g, (copy, here) in enumerate(zip(copies, pieces, strict=True)):
        copy.wait()
        for h in range(2):
            rows = slice(h * 2 * PART, (h + 1) * 2 * PART)
            term = jnp.dot(
                x_buf[rows, here], w_ref[here, :], preferred_element_type=jnp.float32
            )
            if g == 0:
                acc[rows, :] = term
            else:
                write_message((out0, out1)[h], acc[rows, :] + term)


def send_kernel(core, y, arrived, weights, after, out0, out1, acc, *scratch):
    multiply(True, core, y, arrived, weights, *scratch, acc)
    for h, out in enumerate((out0, out1)):
        write_message(out, acc[h * 2 * PART : (h + 1) * 2 * PART, :])


def keep_kernel(core, y, arrived, weights, after, out_ref, *scratch):
    multiply(False, core, y, arrived, weights, *scratch, out_ref)


def half_kernel(leave, core, y_ref, arrived, weights, after, in0, in1, *rest):
    outs, (tok, coef, x_buf) = rest[:-3], rest[-3:]
    y = y_ref[0]
    prepare(core, arrived, tok, coef)
    build((NY - 1 - y, y + 1 - 2 * lax.rem(y, 2)) if leave else (y, y), tok, coef, x_buf)
    acc = jnp.dot(x_buf[...], weights[...], preferred_element_type=jnp.float32)
    for h, ref in enumerate((in0, in1)):
        part = acc[h * PART : (h + 1) * PART, :] + read_message(ref, 1 if leave else 0)
        if leave:
            write_message(outs[h], part)
        else:
            outs[0][h * PART : (h + 1) * PART, :] = part


def middle_kernel(kept, in0, in1, keep_ref, out0, out1):
    for h, (ref, out) in enumerate(((in0, out0), (in1, out1))):
        keep_ref[h * PART : (h + 1) * PART, :] = kept[
            2 * h * PART : (2 * h + 1) * PART, :
        ] + read_message(ref, 0)
        write_message(
            out, kept[(2 * h + 1) * PART : (2 * h + 2) * PART, :] + read_message(ref, 1)
        )


def last_kernel(info, *refs):
    ins, out_ref = refs[:-1], refs[-1]
    width = ins[0].shape[1]
    for q in range(NC):
        kept, messages = ins[3 * q], ins[3 * q + 1 : 3 * q + 3]
        c = lax.rem(info[0] + q, NC)
        for h, ref in enumerate(messages):
            acc = kept[h * PART : (h + 1) * PART, :] + read_message(ref, 0)
            v, code = quantized(acc)
            code = jnp.broadcast_to(code, (PART, 128)).astype(jnp.int32).astype(jnp.int16)
            for j in range(PART // TOK):
                d = (h * (PART // TOK) + j) * NC + c
                here = slice(j * TOK, (j + 1) * TOK)
                out_ref[d, :, 0:width] = v[here, :]
                out_ref[d, :, width : width + 128] = code[here, :]


def final_kernel(ref, bias, out_ref):
    width = out_ref.shape[2] // NC
    for c in range(NC):
        acc = jnp.broadcast_to(bias[:, c * width : (c + 1) * width], (TOK, width))
        for z in range(NZ):
            both = ref[z * NC + c].astype(jnp.int32).astype(jnp.float32)
            scale = jnp.exp(both[:, width : width + 1] * (LN2 / STEP))
            acc = acc + both[:, 0:width] * scale
        out_ref[0, :, c * width : (c + 1) * width] = acc.astype(jnp.bfloat16)


def run(coefficients, block_ids, counts, decoder, bias):
    core = lax.axis_index("c").astype(jnp.int32)
    x = lax.axis_index("x").astype(jnp.int32)
    y = lax.axis_index("y").astype(jnp.int32)
    depth, full = decoder.shape[1], decoder.shape[2]
    width = full // NC
    w_other = lax.ppermute(decoder, "c", ring(NC, 1))

    shape = jax.ShapeDtypeStruct
    packed = call(
        wrap_kernel,
        shape((OWN * (ACTIVE + 1), BLOCK), jnp.bfloat16),
        [HBM, HBM, HBM],
        10,
        scratch=[
            pltpu.SMEM((OWN,), jnp.int32),
            pltpu.VMEM((OWN, ACTIVE, BLOCK), jnp.bfloat16),
            pltpu.VMEM((OWN, ACTIVE), jnp.int32),
            pltpu.SemaphoreType.DMA((3,)),
        ],
    )(counts, coefficients, block_ids)
    parts = [packed]
    for k in range(1, NX):
        parts.append(lax.ppermute(packed, "x", ring(NX, k)))
    outgoing = pl.pallas_call(
        pack_kernel,
        out_shape=shape((CHIPS, ROWS, BLOCK), jnp.bfloat16),
        in_specs=[SMEM] + [VMEM] * NX,
        out_specs=HBM,
        scratch_shapes=[
            pltpu.VMEM((CHIPS, ROWS, BLOCK), jnp.bfloat16),
            pltpu.SemaphoreType.DMA((CHIPS // 4,)),
        ],
        compiler_params=pltpu.CompilerParams(vmem_limit_bytes=10 * MIB),
        name="pack",
    )(x.reshape(1), *parts)
    own = lax.all_to_all(outgoing, ("z", "y"), 0, 0, tiled=True)
    weights = call(
        weights_kernel,
        shape((NC * depth, width), jnp.bfloat16),
        [SMEM, HBM, HBM, ANY],
        WEIGHT_GRANT,
        flops=10**10,
        scratch=[pltpu.SemaphoreType.DMA((PIECES,))],
    )(core.reshape(1), decoder, w_other, outgoing)
    other = lax.ppermute(own, "c", ring(NC, 1))
    pair_a, pair_b = [(i, i ^ 1) for i in range(NY)], [(i, NY - 1 - i) for i in range(NY)]
    place = (core.reshape(1), y.reshape(1))
    message = shape((2 * PART + 8, width), jnp.int16)
    small = shape((PART + 8, width), jnp.int16)

    kept = shape((2 * PART, width), jnp.float32)
    product = {"flops": 2 * 4 * PART * NC * depth * width}
    total = pltpu.VMEM((4 * PART, width), jnp.float32)
    scratch = [
        pltpu.VMEM((CHIPS, SLOTS, BLOCK), jnp.float32),
        pltpu.VMEM((CHIPS, SLOTS, BLOCK), jnp.float32),
        pltpu.VMEM((4 * PART, NC * depth), jnp.bfloat16),
    ]
    given = [SMEM, SMEM, VMEM, VMEM, ANY]

    def cross(m0, m1, pair0, pair1):
        m0 = lax.ppermute(m0, "y", pair0)
        m1 = lax.ppermute(m1, "y", pair1)
        return m0, m1

    m0, m1, weights = call(
        first_kernel,
        [message, message, shape((NC * depth, width), jnp.bfloat16)],
        [SMEM, SMEM, VMEM, HBM],
        FIRST_GRANT,
        scratch=[total, *scratch, pltpu.SemaphoreType.DMA((2,))],
        **product,
    )(*place, own, weights)
    crossing0 = cross(m0, m1, pair_a, pair_b)
    m0, m1 = call(
        send_kernel, [message, message], given, GRANT, scratch=[total] + scratch, **product
    )(*place, other, weights, m0)
    crossing1 = cross(m0, m1, pair_a, pair_b)
    (sums,) = call(
        keep_kernel,
        [shape((4 * PART, width), jnp.float32)],
        given,
        GRANT,
        scratch=scratch,
        **product,
    )(*place, own, weights, m0)
    kept0, m0, m1 = call(middle_kernel, [kept, small, small], [VMEM] * 3, 10)(sums, *crossing0)
    arrived0 = cross(m0, m1, pair_b, pair_a)
    half = scratch[:2] + [pltpu.VMEM((2 * PART, NC * depth), jnp.bfloat16)]

    def second_half(leave, out_shape, after):
        return call(
            functools.partial(half_kernel, leave),
            out_shape,
            given + [VMEM] * 2,
            GRANT,
            flops=2 * 2 * PART * NC * depth * width,
            scratch=half,
        )(*place, other, weights, after, *crossing1)

    m0, m1 = second_half(True, [small, small], m0)
    arrived1 = cross(m0, m1, pair_b, pair_a)
    (kept1,) = second_half(False, [kept], m0)
    out = call(
        last_kernel, shape((NZ * NC, TOK, width + 128), jnp.int16), [SMEM] + [VMEM] * 6, 10
    )(core.reshape(1), kept0, *arrived0, kept1, *arrived1)
    return call(
        final_kernel, shape((1, TOK, full), jnp.bfloat16), [VMEM] * 2, 10
    )(lax.all_to_all(out, ("z", "c"), 0, 0, tiled=True), bias)


def solution(mesh):
    split = Mesh(mesh.devices.reshape(NZ, NY, NC, NX), ("z", "y", "c", "x"))
    lat = ("z", "y", "c")
    in_specs = (
        P((*lat, "x"), None, None),
        P((*lat, "x"), None),
        P((*lat, "x")),
        P(None, lat, "x"),
        P(None, "x"),
    )
    return jax.shard_map(
        run, mesh=split, in_specs=in_specs, out_specs=P(None, lat, "x"), check_vma=False
    )
```
